8 devices in a mesh: model: 2 (over z, y), data: 4 (over x, core).
Axes of the slice: x: 2, y: 2, z: 1, core: 2. Of those that a mesh axis runs over, the one named last changes fastest.
Arguments:
- dec_in: bfloat16 [64, 384, 512], P('data')
- enc_out: bfloat16 [64, 192, 512], P('data')
- grad_out: bfloat16 [64, 384, 512], P('data')
- rel_bias: bfloat16 [32, 6], P(None, 'model')
- self_q: bfloat16 [512, 384], P('data', 'model')
- self_k: bfloat16 [512, 384], P('data', 'model')
- self_v: bfloat16 [512, 384], P('data', 'model')
- self_o: bfloat16 [384, 512], P('model', 'data')
- cross_q: bfloat16 [512, 384], P('data', 'model')
- cross_k: bfloat16 [512, 384], P('data', 'model')
- cross_v: bfloat16 [512, 384], P('data', 'model')
- cross_o: bfloat16 [384, 512], P('model', 'data')
- mlp_wi_0: bfloat16 [512, 1024], P('data', 'model')
- mlp_wi_1: bfloat16 [512, 1024], P('data', 'model')
- mlp_wo: bfloat16 [1024, 512], P('model', 'data')
- norm_self: bfloat16 [512], P('data')
- norm_cross: bfloat16 [512], P('data')
- norm_mlp: bfloat16 [512], P('data')
Outputs:
- output 1: bfloat16 [64, 384, 512], P('data')
- output 2: bfloat16 [64, 384, 512], P('data')
- output 3: bfloat16 [64, 192, 512], P('data')
- output 4: float32 [32, 6], P(None, 'model')
- output 5: float32 [512, 384], P('data', 'model')
- output 6: float32 [512, 384], P('data', 'model')
- output 7: float32 [512, 384], P('data', 'model')
- output 8: float32 [384, 512], P('model', 'data')
- output 9: float32 [512, 384], P('data', 'model')
- output 10: float32 [512, 384], P('data', 'model')
- output 11: float32 [512, 384], P('data', 'model')
- output 12: float32 [384, 512], P('model', 'data')
- output 13: float32 [512, 1024], P('data', 'model')
- output 14: float32 [512, 1024], P('data', 'model')
- output 15: float32 [1024, 512], P('model', 'data')
- output 16: float32 [512], P('data')
- output 17: float32 [512], P('data')
- output 18: float32 [512], P('data')
All inputs are finite; a program needn't handle non-finite values.
Results may differ from the reference program's by a relative error of at most 0.02.
Values are sent between devices in bfloat16 or wider.
A program may use at most 1 GiB of HBM per device.

```python
import math
import jax
import jax.numpy as jnp
from jax import lax

D = 512
HEADS = 6
HEAD = 64
FF = 1024
BATCH = 64
DEC_LEN = 384
ENC_LEN = 192
NUM_BUCKETS = 32
INNER = HEADS * HEAD
EPS = 1e-6
MASK_VALUE = -1e9
BUCKET_EDGES = tuple(math.ceil(16 * 8.0 ** (bucket_no / 16.0)) for bucket_no in range(1, 16))


def setup_inputs(seed: int = 0) -> dict:
    key_list = jax.random.split(jax.random.key(seed), 18)

    def normal(slot, arr_shape, factor):
        return (jax.random.normal(key_list[slot], arr_shape, jnp.float32) * factor).astype(jnp.bfloat16)

    def gain_draw(slot):
        return (1.0 + 0.3 * jax.random.normal(key_list[slot], (D,), jnp.float32)).astype(jnp.bfloat16)

    in_scale = D ** -0.5
    q_scale = (D * HEAD) ** -0.5
    out_scale = INNER ** -0.5
    return {
        "dec_in": normal(0, (BATCH, DEC_LEN, D), 1.0),
        "enc_out": normal(1, (BATCH, ENC_LEN, D), 1.0),
        "grad_out": normal(2, (BATCH, DEC_LEN, D), 1.0),
        "rel_bias": normal(3, (NUM_BUCKETS, HEADS), 1.5),
        "self_q": normal(4, (D, INNER), q_scale),
        "self_k": normal(5, (D, INNER), in_scale),
        "self_v": normal(6, (D, INNER), in_scale),
        "self_o": normal(7, (INNER, D), out_scale),
        "cross_q": normal(8, (D, INNER), q_scale),
        "cross_k": normal(9, (D, INNER), in_scale),
        "cross_v": normal(10, (D, INNER), in_scale),
        "cross_o": normal(11, (INNER, D), out_scale),
        "mlp_wi_0": normal(12, (D, FF), in_scale),
        "mlp_wi_1": normal(13, (D, FF), in_scale),
        "mlp_wo": normal(14, (FF, D), FF ** -0.5),
        "norm_self": gain_draw(15),
        "norm_cross": gain_draw(16),
        "norm_mlp": gain_draw(17),
    }


def to_bf(value_in):
    return value_in.astype(jnp.bfloat16).astype(jnp.float32)


def rms_norm(act_in, gain_vec):
    inv_rms = lax.rsqrt(jnp.mean(act_in * act_in, axis=-1, keepdims=True) + EPS)
    return to_bf(act_in * inv_rms * gain_vec)


def bucket_ids(seq_len):
    positions = jnp.arange(seq_len)
    rel_dist = jnp.maximum(positions[:, None] - positions[None, :], 0)
    bucket_edges = jnp.array(BUCKET_EDGES, dtype=jnp.int32)
    return jnp.minimum(rel_dist, 16) + jnp.sum((rel_dist[:, :, None] >= bucket_edges).astype(jnp.int32), axis=-1)


def project(act_in, weight):
    return to_bf(jnp.dot(act_in, weight, preferred_element_type=jnp.float32)).reshape(act_in.shape[0], HEADS, HEAD)


def attention(q_heads, k_heads, v_heads, pos_bias, key_mask):
    logits = to_bf(jnp.einsum("qhe,khe->hqk", q_heads, k_heads)) + pos_bias
    logits = jnp.where(key_mask, logits, MASK_VALUE)
    attn_probs = to_bf(jax.nn.softmax(logits, axis=-1))
    context = to_bf(jnp.einsum("hqk,khe->qhe", attn_probs, v_heads))
    return context.reshape(q_heads.shape[0], INNER)


def layer_seq(dec_seq, enc_seq, params):
    (rel_bias, self_q, self_k, self_v, self_o, cross_q, cross_k, cross_v, cross_o,
     mlp_wi_0, mlp_wi_1, mlp_wo, norm_self, norm_cross, norm_mlp) = params
    positions = jnp.arange(DEC_LEN)
    causal = positions[:, None] >= positions[None, :]
    pos_bias = jnp.transpose(rel_bias[bucket_ids(DEC_LEN)], (2, 0, 1))
    normed_1 = rms_norm(dec_seq, norm_self)
    ctx_self = attention(project(normed_1, self_q), project(normed_1, self_k), project(normed_1, self_v), pos_bias, causal)
    mid_1 = to_bf(dec_seq + jnp.dot(ctx_self, self_o, preferred_element_type=jnp.float32))
    normed_2 = rms_norm(mid_1, norm_cross)
    ctx_cross = attention(project(normed_2, cross_q), project(enc_seq, cross_k), project(enc_seq, cross_v), 0.0, True)
    mid_2 = to_bf(mid_1 + jnp.dot(ctx_cross, cross_o, preferred_element_type=jnp.float32))
    normed_3 = rms_norm(mid_2, norm_mlp)
    pre_0 = to_bf(jnp.dot(normed_3, mlp_wi_0, preferred_element_type=jnp.float32))
    pre_1 = to_bf(jnp.dot(normed_3, mlp_wi_1, preferred_element_type=jnp.float32))
    hidden = to_bf(jax.nn.gelu(pre_0, approximate=True) * pre_1)
    return to_bf(mid_2 + jnp.dot(hidden, mlp_wo, preferred_element_type=jnp.float32))


def reference(dec_in, enc_out, grad_out, rel_bias, self_q, self_k, self_v, self_o, cross_q, cross_k, cross_v, cross_o, mlp_wi_0, mlp_wi_1, mlp_wo, norm_self, norm_cross, norm_mlp):
    params = tuple(param_arr.astype(jnp.float32) for param_arr in (rel_bias, self_q, self_k, self_v, self_o, cross_q, cross_k, cross_v, cross_o, mlp_wi_0, mlp_wi_1, mlp_wo, norm_self, norm_cross, norm_mlp))

    def batch_step(grad_acc, seq_item):
        dec_seq, enc_seq, dy_seq = seq_item
        out_seq, pull_back = jax.vjp(layer_seq, dec_seq.astype(jnp.float32), enc_seq.astype(jnp.float32), params)
        d_dec, d_enc, d_params = pull_back(dy_seq.astype(jnp.float32))
        grad_acc = jax.tree.map(jnp.add, grad_acc, d_params)
        return grad_acc, (out_seq.astype(jnp.bfloat16), d_dec.astype(jnp.bfloat16), d_enc.astype(jnp.bfloat16))

    grad_zero = jax.tree.map(jnp.zeros_like, params)
    grad_sums, (dec_out, grad_dec, grad_enc) = lax.scan(batch_step, grad_zero, (dec_in, enc_out, grad_out))
    (g_bias, g_self_q, g_self_k, g_self_v, g_self_o, g_cross_q, g_cross_k, g_cross_v, g_cross_o,
     g_wi_0, g_wi_1, g_mlp_wo, g_norm_self, g_norm_cross, g_norm_mlp) = grad_sums
    return (dec_out, grad_dec, grad_enc, g_bias, g_self_q, g_self_k, g_self_v, g_self_o, g_cross_q, g_cross_k, g_cross_v, g_cross_o, g_wi_0, g_wi_1, g_mlp_wo, g_norm_self, g_norm_cross, g_norm_mlp)
```

```python
import functools
import math
import jax
import jax.numpy as jnp
from jax import lax
from jax.experimental import pallas as pl
from jax.experimental.pallas import tpu as pltpu
from jax.sharding import PartitionSpec as P

EPS = 1e-6
BUCKET_EDGES = tuple(math.ceil(16 * 8.0 ** (bucket_no / 16.0)) for bucket_no in range(1, 16))
NUM_BUCKETS = 32
D, INNER, FF = 512, 384, 1024
T, E = 384, 192
PAIRS, BLK = 3, 128
ROW_OFF = (0, 128, 384)
F32, BF = jnp.float32, jnp.bfloat16
GELU_C = math.sqrt(2.0 / math.pi)
VMEM_LIMIT = 60 * 1024 * 1024


def nn(lhs, rhs):
    return lax.dot_general(lhs, rhs, (((1,), (0,)), ((), ())), preferred_element_type=F32)


def nt(lhs, rhs):
    return lax.dot_general(lhs, rhs, (((1,), (1,)), ((), ())), preferred_element_type=F32)


def tn(lhs, rhs):
    return lax.dot_general(lhs, rhs, (((0,), (0,)), ((), ())), preferred_element_type=F32)


def bf(val):
    return val.astype(BF)


def rounded(val):
    return val.astype(BF).astype(F32)


def unit_norm(act):
    act_f = act.astype(F32)
    inv_rms = lax.rsqrt(jnp.mean(act_f * act_f, axis=-1, keepdims=True) + EPS)
    return act_f * inv_rms, inv_rms


def norm_back(d_norm, unit_act, inv_rms, gain):
    d_norm_f = rounded(d_norm)
    d_unit = d_norm_f * gain
    d_act = inv_rms * (d_unit - unit_act * jnp.mean(d_unit * unit_act, axis=-1, keepdims=True))
    return d_act, jnp.sum(d_norm_f * unit_act, axis=0, keepdims=True)


def half_masks():
    lane = lax.broadcasted_iota(jnp.int32, (1, BLK), 1)
    low = jnp.where(lane < 64, 1.0, 0.0)
    return bf(low), bf(1.0 - low), lane < 64


def pick_half(low_rows, high_rows):
    lane = lax.broadcasted_iota(jnp.int32, low_rows.shape, 1)
    return jnp.where(lane < 64, low_rows, high_rows)


def unpack_weights(pack_ref, w_ref):
    for row in range(4):
        for mat in range(4):
            parts = [pack_ref[4 * half + row, :, mat * 192:(mat + 1) * 192] for half in range(2)]
            w_ref[row * BLK:(row + 1) * BLK, mat * INNER:(mat + 1) * INNER] = jnp.concatenate(parts, axis=1)


def pack_grads(acc_ref, out_ref):
    for row in range(4):
        for half in range(2):
            parts = [acc_ref[row * BLK:(row + 1) * BLK, mat * INNER + half * 192:mat * INNER + half * 192 + 192] for mat in range(4)]
            out_ref[4 * half + row] = jnp.concatenate(parts, axis=1)


def bucket_block(diag):
    row = lax.broadcasted_iota(jnp.int32, (BLK, BLK), 0)
    col = lax.broadcasted_iota(jnp.int32, (BLK, BLK), 1)
    rel = row - col + diag * BLK
    bucket = jnp.clip(rel, 0, 16)
    for edge in BUCKET_EDGES:
        bucket = bucket + jnp.where(rel >= edge, 1, 0)
    return rel, bucket


def build_bias(table_ref, bias_ref):
    for diag in range(3):
        rel, bucket = bucket_block(diag)
        for head in range(6):
            row = jnp.broadcast_to(table_ref[head:head + 1, :], (BLK, BLK))
            vals = jnp.take_along_axis(row, bucket, axis=1, mode="promise_in_bounds")
            bias_ref[head, diag] = jnp.where(rel >= 0, vals, -jnp.inf)


def self_fwd(part_ref, pack_ref, gain_ref, table_ref, x_ref, x1_ref, qkv_ref, p_ref, ctx_ref, w_ref, bias_ref):
    @pl.when(pl.program_id(0) == 0)
    def _():
        unpack_weights(pack_ref, w_ref)
        build_bias(table_ref, bias_ref)

    low, high, _ = half_masks()
    x_in = x_ref[0]
    unit_act, _ = unit_norm(x_in)
    normed = bf(unit_act * gain_ref[0:1, :])
    qkv_ref[0] = bf(nn(normed, w_ref[:, :3 * INNER]))
    for pair in range(PAIRS):
        lanes = pl.ds(pair * BLK, BLK)
        q_pair = qkv_ref[0, :, pl.ds(pair * BLK, BLK)]
        k_pair = qkv_ref[0, :, pl.ds(INNER + pair * BLK, BLK)]
        v_pair = qkv_ref[0, :, pl.ds(2 * INNER + pair * BLK, BLK)]
        k_heads = (k_pair * low, k_pair * high)
        v_heads = (v_pair * low, v_pair * high)
        for blk in range(3):
            keys = (blk + 1) * BLK
            q_rows = q_pair[blk * BLK:(blk + 1) * BLK]
            probs = []
            for sub in range(2):
                head = 2 * pair + sub
                bias = jnp.concatenate([bias_ref[head, blk - key_blk] for key_blk in range(blk + 1)], axis=1)
                logits = rounded(nt(q_rows, k_heads[sub][:keys])) + bias
                expd = jnp.exp(logits - jnp.max(logits, axis=1, keepdims=True))
                prob = expd * (1.0 / jnp.sum(expd, axis=1, keepdims=True))
                p_ref[0, head, :, ROW_OFF[blk]:ROW_OFF[blk] + keys] = prob
                probs.append(bf(prob))
            context = nn(jnp.concatenate(probs, axis=1), jnp.concatenate([v_heads[0][:keys], v_heads[1][:keys]], axis=0))
            ctx_ref[0, blk * BLK:(blk + 1) * BLK, lanes] = bf(context)
    x1_ref[0] = bf(x_in.astype(F32) + nt(ctx_ref[0], w_ref[:, 3 * INNER:]))


def cross_mlp(part_ref, pack_ref, mlp_ref, gain_ref, x1_ref, enc_ref, dy_ref,
              y_ref, dmid_ref, q_ref, kv_ref, p_ref, ctx_ref, dmlp_ref, dgain_ref,
              w_ref, hid_ref, dpre_ref):
    @pl.when(pl.program_id(0) == 0)
    def _():
        unpack_weights(pack_ref, w_ref)
        dmlp_ref[...] = jnp.zeros_like(dmlp_ref)
        dgain_ref[...] = jnp.zeros_like(dgain_ref)

    low, high, _ = half_masks()
    unit_act, _ = unit_norm(x1_ref[0])
    normed = bf(unit_act * gain_ref[1:2, :])
    q_ref[0] = bf(nn(normed, w_ref[:, :INNER]))
    kv_ref[0] = bf(nn(enc_ref[0], w_ref[:, INNER:3 * INNER]))
    for pair in range(PAIRS):
        lanes = pl.ds(pair * BLK, BLK)
        q_pair = q_ref[0, :, lanes]
        k_pair = kv_ref[0, :, lanes]
        v_pair = kv_ref[0, :, pl.ds(INNER + pair * BLK, BLK)]
        k_heads = (k_pair * low, k_pair * high)
        probs = []
        for sub in range(2):
            logits = rounded(nt(k_heads[sub], q_pair))
            expd = jnp.exp(logits - jnp.max(logits, axis=0, keepdims=True))
            prob = expd * (1.0 / jnp.sum(expd, axis=0, keepdims=True))
            p_ref[0, 2 * pair + sub] = prob
            probs.append(bf(prob))
        context = tn(jnp.concatenate(probs, axis=0), jnp.concatenate([v_pair * low, v_pair * high], axis=0))
        ctx_ref[0, :, lanes] = bf(context)
    mid_2 = rounded(x1_ref[0].astype(F32) + nt(ctx_ref[0], w_ref[:, 3 * INNER:]))

    unit_3, inv_3 = unit_norm(mid_2)
    gain_3 = gain_ref[2:3, :]
    normed_3 = bf(unit_3 * gain_3)
    dy = dy_ref[0]
    out = mid_2
    d_norm = jnp.zeros((T, D), F32)
    for half in range(2):
        wi_0 = mlp_ref[half, :, 0:512]
        wi_1 = mlp_ref[half, :, 512:1024]
        wo_t = mlp_ref[half, :, 1024:1536]
        pre_0 = rounded(nn(normed_3, wi_0))
        pre_1 = rounded(nn(normed_3, wi_1))
        d_hid = rounded(nn(dy, wo_t))
        sq = pre_0 * pre_0
        tanh = jnp.tanh(GELU_C * (pre_0 + 0.044715 * (sq * pre_0)))
        cdf = 0.5 * (1.0 + tanh)
        gelu = pre_0 * cdf
        slope = cdf + (0.5 * pre_0) * (1.0 - tanh * tanh) * (GELU_C * (1.0 + (3.0 * 0.044715) * sq))
        hid_ref[...] = bf(gelu * pre_1)
        dpre_ref[:, 0:512] = bf((d_hid * pre_1) * slope)
        dpre_ref[:, 512:1024] = bf(d_hid * gelu)
        out = out + nt(hid_ref[...], wo_t)
        d_norm = d_norm + nt(dpre_ref[...], mlp_ref[half, :, 0:1024])
        dmlp_ref[half, :, 0:1024] += tn(normed_3, dpre_ref[...])
        dmlp_ref[half, :, 1024:1536] += tn(dy, hid_ref[...])
    y_ref[0] = bf(out)
    d_act, d_gain = norm_back(d_norm, unit_3, inv_3, gain_3)
    dgain_ref[...] += jnp.broadcast_to(d_gain, (8, D))
    dmid_ref[0] = bf(dy.astype(F32) + d_act)


def cross_bwd(part_ref, pack_ref, gain_ref, x1_ref, enc_ref, dmid_ref, q_ref, kv_ref, p_ref, ctx_ref,
              dx1_ref, denc_ref, dw_ref, dgain_ref, w_ref, acc_ref, dq_ref, dkv_ref, dctx_ref):
    step = pl.program_id(0)

    @pl.when(step == 0)
    def _():
        unpack_weights(pack_ref, w_ref)
        acc_ref[...] = jnp.zeros_like(acc_ref)
        dgain_ref[...] = jnp.zeros_like(dgain_ref)

    low, high, _ = half_masks()
    d_mid = dmid_ref[0]
    dctx_ref[...] = bf(nn(d_mid, w_ref[:, 3 * INNER:]))
    acc_ref[:, 3 * INNER:] += tn(d_mid, ctx_ref[0])
    for pair in range(PAIRS):
        lanes = pl.ds(pair * BLK, BLK)
        q_pair = q_ref[0, :, lanes]
        k_pair = kv_ref[0, :, lanes]
        v_pair = kv_ref[0, :, pl.ds(INNER + pair * BLK, BLK)]
        dctx_pair = dctx_ref[:, lanes]
        v_heads = (v_pair * low, v_pair * high)
        probs, d_logits = [], []
        for sub in range(2):
            prob = p_ref[0, 2 * pair + sub]
            d_prob = rounded(nt(v_heads[sub], dctx_pair))
            delta = jnp.sum(prob * d_prob, axis=0, keepdims=True)
            d_logits.append(bf(prob * (d_prob - delta)))
            probs.append(bf(prob))
        d_logit = jnp.concatenate(d_logits, axis=0)
        dq_ref[:, lanes] = bf(tn(d_logit, jnp.concatenate([k_pair * low, k_pair * high], axis=0)))
        dk_both = nn(d_logit, q_pair)
        dkv_ref[:, lanes] = bf(pick_half(dk_both[:E], dk_both[E:]))
        dv_both = nn(jnp.concatenate(probs, axis=0), dctx_pair)
        dkv_ref[:, pl.ds(INNER + pair * BLK, BLK)] = bf(pick_half(dv_both[:E], dv_both[E:]))
    denc_ref[0] = bf(nt(dkv_ref[...], w_ref[:, INNER:3 * INNER]))
    acc_ref[:, INNER:3 * INNER] += tn(enc_ref[0], dkv_ref[...])
    unit_act, inv_rms = unit_norm(x1_ref[0])
    gain = gain_ref[1:2, :]
    acc_ref[:, :INNER] += tn(bf(unit_act * gain), dq_ref[...])
    d_act, d_gain = norm_back(nt(dq_ref[...], w_ref[:, :INNER]), unit_act, inv_rms, gain)
    dgain_ref[...] += jnp.broadcast_to(d_gain, (8, D))
    dx1_ref[0] = bf(d_mid.astype(F32) + d_act)

    @pl.when(step == pl.num_programs(0) - 1)
    def _():
        pack_grads(acc_ref, dw_ref)


def self_bwd(part_ref, pack_ref, gain_ref, x_ref, dmid_ref, qkv_ref, p_ref, ctx_ref,
             dx_ref, dw_ref, dgain_ref, dbias_ref, w_ref, acc_ref, dqkv_ref, dctx_ref):
    step = pl.program_id(0)

    @pl.when(step == 0)
    def _():
        unpack_weights(pack_ref, w_ref)
        acc_ref[...] = jnp.zeros_like(acc_ref)
        dgain_ref[...] = jnp.zeros_like(dgain_ref)
        dbias_ref[...] = jnp.zeros_like(dbias_ref)

    low, high, _ = half_masks()
    d_mid = dmid_ref[0]
    dctx_ref[...] = bf(nn(d_mid, w_ref[:, 3 * INNER:]))
    acc_ref[:, 3 * INNER:] += tn(d_mid, ctx_ref[0])
    for pair in range(PAIRS):
        q_pair = qkv_ref[0, :, pl.ds(pair * BLK, BLK)]
        k_pair = qkv_ref[0, :, pl.ds(INNER + pair * BLK, BLK)]
        v_pair = qkv_ref[0, :, pl.ds(2 * INNER + pair * BLK, BLK)]
        dctx_pair = dctx_ref[:, pl.ds(pair * BLK, BLK)]
        k_heads = (k_pair * low, k_pair * high)
        v_heads = (v_pair * low, v_pair * high)
        probs, d_logits = [[], []], [[], []]
        for blk in range(3):
            keys = (blk + 1) * BLK
            for sub in range(2):
                head = 2 * pair + sub
                prob = p_ref[0, head, :, ROW_OFF[blk]:ROW_OFF[blk] + keys]
                d_prob = rounded(nt(dctx_pair[blk * BLK:(blk + 1) * BLK], v_heads[sub][:keys]))
                delta = jnp.sum(prob * d_prob, axis=1, keepdims=True)
                d_logit = prob * (d_prob - delta)
                for key_blk in range(blk + 1):
                    dbias_ref[head, blk - key_blk] += d_logit[:, key_blk * BLK:(key_blk + 1) * BLK]
                d_logits[sub].append(bf(d_logit))
                probs[sub].append(bf(prob))
            d_query = nn(jnp.concatenate([d_logits[0][blk], d_logits[1][blk]], axis=1),
                         jnp.concatenate([k_heads[0][:keys], k_heads[1][:keys]], axis=0))
            dqkv_ref[blk * BLK:(blk + 1) * BLK, pl.ds(pair * BLK, BLK)] = bf(d_query)
        for vals, rhs, base in ((d_logits, q_pair, INNER), (probs, dctx_pair, 2 * INNER)):
            for key_blk in range(3):
                cols = slice(key_blk * BLK, (key_blk + 1) * BLK)
                left = jnp.concatenate([jnp.concatenate([vals[sub][blk][:, cols] for blk in range(key_blk, 3)], axis=0) for sub in range(2)], axis=1)
                both = tn(left, rhs[key_blk * BLK:])
                dqkv_ref[cols, pl.ds(base + pair * BLK, BLK)] = bf(pick_half(both[:BLK], both[BLK:]))
    unit_act, inv_rms = unit_norm(x_ref[0])
    gain = gain_ref[0:1, :]
    acc_ref[:, :3 * INNER] += tn(bf(unit_act * gain), dqkv_ref[...])
    d_act, d_gain = norm_back(nt(dqkv_ref[...], w_ref[:, :3 * INNER]), unit_act, inv_rms, gain)
    dgain_ref[...] += jnp.broadcast_to(d_gain, (8, D))
    dx_ref[0] = bf(d_mid.astype(F32) + d_act)

    @pl.when(step == pl.num_programs(0) - 1)
    def _():
        pack_grads(acc_ref, dw_ref)


def bucket_sums(dbias_ref, dg1_ref, dg2_ref, dg3_ref, out_ref):
    blocks = [bucket_block(diag) for diag in range(3)]
    buckets = [jnp.where(rel >= 0, bucket, -1) for rel, bucket in blocks]

    lane = lax.broadcasted_iota(jnp.int32, (8, BLK), 1)

    def one_bucket(bucket_no, sums):
        rows = []
        for head in range(6):
            total = jnp.zeros((BLK, BLK), F32)
            for diag in range(3):
                total = total + jnp.where(buckets[diag] == bucket_no, dbias_ref[head, diag], 0.0)
            rows.append(jnp.sum(total, axis=0, keepdims=True))
        rows += [jnp.zeros((1, BLK), F32)] * 2
        per_head = jnp.sum(jnp.concatenate(rows, axis=0), axis=1, keepdims=True)
        return jnp.where(lane == bucket_no, per_head, sums)

    out_ref[:, D:] = lax.fori_loop(0, NUM_BUCKETS, one_bucket, jnp.zeros((8, BLK), F32))
    row = lax.broadcasted_iota(jnp.int32, (8, D), 0)
    out_ref[:, :D] = jnp.where(row == 0, dg1_ref[...], jnp.where(row == 1, dg2_ref[...], dg3_ref[...]))


def seq_block(*dims):
    zeros = (0,) * len(dims)
    return pl.BlockSpec((1,) + dims, lambda i, part: (i,) + zeros)


def arg_block(*dims):
    zeros = (0,) * len(dims)
    return pl.BlockSpec((1,) + dims, lambda i, part: (part[0] * 8 + i,) + zeros)


def whole(*dims):
    zeros = (0,) * len(dims)
    return pl.BlockSpec(dims, lambda i, part: zeros)


def call(body, name, seqs, flops, in_specs, outs, scratch, *args):
    out_specs, out_shape = zip(*outs)
    return pl.pallas_call(
        body,
        name=name,
        out_shape=out_shape,
        grid_spec=pltpu.PrefetchScalarGridSpec(num_scalar_prefetch=1, grid=(seqs,), in_specs=in_specs, out_specs=out_specs, scratch_shapes=scratch),
        compiler_params=pltpu.CompilerParams(dimension_semantics=("arbitrary",), vmem_limit_bytes=VMEM_LIMIT),
        cost_estimate=pl.CostEstimate(flops=flops, bytes_accessed=40_000_000, transcendentals=0),
    )(*args)


def shape(dims, dtype):
    return jax.ShapeDtypeStruct(dims, dtype)


def seq_out(seqs, dims, dtype):
    return seq_block(*dims), shape((seqs,) + dims, dtype)


def whole_out(dims, dtype):
    return whole(*dims), shape(dims, dtype)


def layer_shard(dec_in, enc_out, grad_out, rel_bias, self_q, self_k, self_v, self_o, cross_q, cross_k, cross_v, cross_o, mlp_wi_0, mlp_wi_1, mlp_wo, norm_self, norm_cross, norm_mlp):
    axes = ("model", "data")
    seqs = dec_in.shape[0] // 2
    part = lax.axis_index("model").astype(jnp.int32).reshape(1)
    rows = (norm_self[None], norm_cross[None], norm_mlp[None], jnp.pad(rel_bias.T, ((0, 0), (0, BLK - NUM_BUCKETS))))
    small = sum(jnp.pad(val, ((pos, 16 - pos - val.shape[0]), (0, 0))) for pos, val in enumerate(rows))
    small = lax.all_gather(small, axes).astype(F32)
    gains = small[:4].transpose(1, 0, 2).reshape(16, D)[:8]
    table = small[:, 3:6].reshape(2, 4, 3, BLK)[:, 0].reshape(6, BLK)
    table = jnp.pad(table, ((0, 2), (0, 0)))
    w_self = lax.all_gather(jnp.concatenate([self_q, self_k, self_v, self_o.T], axis=1), axes)
    w_cross = lax.all_gather(jnp.concatenate([cross_q, cross_k, cross_v, cross_o.T], axis=1), axes)
    w_mlp = lax.all_gather(jnp.concatenate([mlp_wi_0, mlp_wi_1, mlp_wo.T], axis=1), axes).reshape(2, D, 1536)

    vmem = pltpu.VMEM
    pack_spec = whole(8, BLK, 768)
    w_scr = vmem((D, 1536), BF)
    acc_scr = vmem((D, 1536), F32)
    mid_1, qkv, probs, ctx = call(
        self_fwd, "self_fwd", seqs, 60_000_000_000,
        [pack_spec, whole(8, D), whole(8, BLK), arg_block(T, D)],
        [seq_out(seqs, (T, D), BF), seq_out(seqs, (T, 3 * INNER), BF), seq_out(seqs, (6, BLK, 768), F32), seq_out(seqs, (T, INNER), BF)],
        [w_scr, vmem((6, 3, BLK, BLK), F32)],
        part, w_self, gains, table, dec_in)
    dec_out, d_mid_2, q_x, kv_x, probs_x, ctx_x, d_mlp, d_gain_3 = call(
        cross_mlp, "cross_mlp", seqs, 120_000_000_000,
        [pack_spec, whole(2, D, 1536), whole(8, D), seq_block(T, D), arg_block(E, D), arg_block(T, D)],
        [seq_out(seqs, (T, D), BF), seq_out(seqs, (T, D), BF), seq_out(seqs, (T, INNER), BF), seq_out(seqs, (E, 2 * INNER), BF),
         seq_out(seqs, (6, E, T), F32), seq_out(seqs, (T, INNER), BF), whole_out((2, D, 1536), F32), whole_out((8, D), F32)],
        [w_scr, vmem((T, 512), BF), vmem((T, 1024), BF)],
        part, w_cross, w_mlp, gains, mid_1, enc_out, grad_out)
    dec_out = lax.all_gather(dec_out, "model", axis=0, tiled=True)
    d_mlp = lax.psum_scatter(d_mlp.reshape(8, BLK, 1536), axes, scatter_dimension=0)
    d_mid_1, grad_enc, d_cross, d_gain_2 = call(
        cross_bwd, "cross_bwd", seqs, 60_000_000_000,
        [pack_spec, whole(8, D), seq_block(T, D), arg_block(E, D), seq_block(T, D), seq_block(T, INNER), seq_block(E, 2 * INNER), seq_block(6, E, T), seq_block(T, INNER)],
        [seq_out(seqs, (T, D), BF), seq_out(seqs, (E, D), BF), whole_out((8, BLK, 768), F32), whole_out((8, D), F32)],
        [w_scr, acc_scr, vmem((T, INNER), BF), vmem((E, 2 * INNER), BF), vmem((T, INNER), BF)],
        part, w_cross, gains, mid_1, enc_out, d_mid_2, q_x, kv_x, probs_x, ctx_x)
    grad_enc = lax.all_gather(grad_enc, "model", axis=0, tiled=True)
    d_cross = lax.psum_scatter(d_cross, axes, scatter_dimension=0)
    grad_dec, d_self, d_gain_1, d_bias = call(
        self_bwd, "self_bwd", seqs, 90_000_000_000,
        [pack_spec, whole(8, D), arg_block(T, D), seq_block(T, D), seq_block(T, 3 * INNER), seq_block(6, BLK, 768), seq_block(T, INNER)],
        [seq_out(seqs, (T, D), BF), whole_out((8, BLK, 768), F32), whole_out((8, D), F32), whole_out((6, 3, BLK, BLK), F32)],
        [w_scr, acc_scr, vmem((T, 3 * INNER), BF), vmem((T, INNER), BF)],
        part, w_self, gains, dec_in, d_mid_1, qkv, probs, ctx)
    grad_dec = lax.all_gather(grad_dec, "model", axis=0, tiled=True)
    d_self = lax.psum_scatter(d_self, axes, scatter_dimension=0)
    tiny = pl.pallas_call(bucket_sums, name="bucket_sums", out_shape=shape((8, D + BLK), F32))(d_bias, d_gain_1, d_gain_2, d_gain_3)
    tiny = lax.psum(tiny, axes)
    data_no, model_no = lax.axis_index("data"), lax.axis_index("model")
    gain_grads = lax.dynamic_slice(tiny, (0, data_no * BLK), (3, BLK))
    gain_grads = (gain_grads[0], gain_grads[1], gain_grads[2])
    bias_sums = tiny[:, D:D + NUM_BUCKETS]
    grad_bias = jnp.where(model_no == 0, bias_sums[0:3], bias_sums[3:6]).T

    def split_attn(grad_pack):
        mats = [grad_pack[:, 192 * pos:192 * (pos + 1)] for pos in range(4)]
        return mats[0], mats[1], mats[2], mats[3].T

    return (dec_out, grad_dec, grad_enc, grad_bias) + split_attn(d_self) + split_attn(d_cross) + (
        d_mlp[:, 0:512], d_mlp[:, 512:1024], d_mlp[:, 1024:1536].T) + gain_grads


def solution(mesh):
    row_spec = P("data", None, None)
    col_in = P("data", "model")
    col_out = P("model", "data")
    gain_spec = P("data")
    bias_spec = P(None, "model")
    arg_specs = (row_spec, row_spec, row_spec, bias_spec, col_in, col_in, col_in, col_out, col_in, col_in, col_in, col_out, col_in, col_in, col_out, gain_spec, gain_spec, gain_spec)
    out_specs = (row_spec, row_spec, row_spec) + arg_specs[3:]
    return jax.shard_map(layer_shard, mesh=mesh, in_specs=arg_specs, out_specs=out_specs, check_vma=False)
```

```python
import functools
import math
import jax
import jax.numpy as jnp
from jax import lax
from jax.experimental import pallas as pl
from jax.experimental.pallas import tpu as pltpu
from jax.sharding import PartitionSpec as P

EPS = 1e-6
BUCKET_EDGES = tuple(math.ceil(16 * 8.0 ** (bucket_no / 16.0)) for bucket_no in range(1, 16))
NUM_BUCKETS = 32
D, INNER = 512, 384
T, E = 384, 192
PAIRS, BLK = 3, 128
ROW_OFF = (0, 128, 384)
F32, BF = jnp.float32, jnp.bfloat16
GELU_C = math.sqrt(2.0 / math.pi)
VMEM_LIMIT = 60 * 1024 * 1024


def nn(lhs, rhs):
    return lax.dot_general(lhs, rhs, (((1,), (0,)), ((), ())), preferred_element_type=F32)


def nt(lhs, rhs):
    return lax.dot_general(lhs, rhs, (((1,), (1,)), ((), ())), preferred_element_type=F32)


def tn(lhs, rhs):
    return lax.dot_general(lhs, rhs, (((0,), (0,)), ((), ())), preferred_element_type=F32)


def bf(val):
    return val.astype(BF)


def rounded(val):
    return val.astype(BF).astype(F32)


def unit_norm(act):
    act_f = act.astype(F32)
    inv_rms = lax.rsqrt(jnp.mean(act_f * act_f, axis=-1, keepdims=True) + EPS)
    return act_f * inv_rms, inv_rms


def norm_back(d_norm, unit_act, inv_rms, gain):
    d_norm_f = rounded(d_norm)
    d_unit = d_norm_f * gain
    d_act = inv_rms * (d_unit - unit_act * jnp.mean(d_unit * unit_act, axis=-1, keepdims=True))
    return d_act, jnp.sum(d_norm_f * unit_act, axis=0, keepdims=True)


def half_masks():
    lane = lax.broadcasted_iota(jnp.int32, (1, BLK), 1)
    low = jnp.where(lane < 64, 1.0, 0.0)
    return bf(low), bf(1.0 - low), lane < 64


def pick_half(low_rows, high_rows):
    lane = lax.broadcasted_iota(jnp.int32, low_rows.shape, 1)
    return jnp.where(lane < 64, low_rows, high_rows)


def pack_slots():
    for row in range(4):
        for half in range(2):
            for mat in range(4):
                first = mat * INNER + half * 192
                yield 4 * half + row, slice(mat * 192, (mat + 1) * 192), slice(first, first + 192), slice(row * BLK, (row + 1) * BLK)


def unpack(pack_ref, full_ref):
    for dev, rows, feats, cols in pack_slots():
        full_ref[feats, cols] = pack_ref[dev, rows, :]


def repack(full_ref, pack_ref):
    for dev, rows, feats, cols in pack_slots():
        pack_ref[dev, rows, :] = full_ref[feats, cols]


def bucket_block(diag):
    row = lax.broadcasted_iota(jnp.int32, (BLK, BLK), 0)
    col = lax.broadcasted_iota(jnp.int32, (BLK, BLK), 1)
    rel = row - col + diag * BLK
    bucket = jnp.clip(rel, 0, 16)
    for edge in BUCKET_EDGES:
        bucket = bucket + jnp.where(rel >= edge, 1, 0)
    return rel, bucket


def build_bias(table_ref, bias_ref):
    for diag in range(3):
        rel, bucket = bucket_block(diag)
        for head in range(6):
            row = jnp.broadcast_to(table_ref[head:head + 1, :], (BLK, BLK))
            vals = jnp.take_along_axis(row, bucket, axis=1, mode="promise_in_bounds")
            bias_ref[head, diag] = jnp.where(rel >= 0, vals, -jnp.inf)


def self_fwd(part_ref, pack_ref, gain_ref, table_ref, x_ref, x1_ref, qkv_ref, p_ref, ctx_ref, w_ref, bias_ref):
    @pl.when(pl.program_id(0) == 0)
    def _():
        unpack(pack_ref, w_ref)
        build_bias(table_ref, bias_ref)

    low, high, _ = half_masks()
    x_in = x_ref[0]
    unit_act, _ = unit_norm(x_in)
    normed = bf(unit_act * gain_ref[0:1, :])
    qkv_ref[0] = bf(nt(normed, w_ref[:3 * INNER]))
    for pair in range(PAIRS):
        lanes = pl.ds(pair * BLK, BLK)
        q_pair = qkv_ref[0, :, pl.ds(pair * BLK, BLK)]
        k_pair = qkv_ref[0, :, pl.ds(INNER + pair * BLK, BLK)]
        v_pair = qkv_ref[0, :, pl.ds(2 * INNER + pair * BLK, BLK)]
        k_heads = (k_pair * low, k_pair * high)
        v_heads = (v_pair * low, v_pair * high)
        for blk in range(3):
            keys = (blk + 1) * BLK
            q_rows = q_pair[blk * BLK:(blk + 1) * BLK]
            probs = []
            for sub in range(2):
                head = 2 * pair + sub
                bias = jnp.concatenate([bias_ref[head, blk - key_blk] for key_blk in range(blk + 1)], axis=1)
                logits = rounded(nt(q_rows, k_heads[sub][:keys])) + bias
                expd = jnp.exp(logits - jnp.max(logits, axis=1, keepdims=True))
                prob = expd * (1.0 / jnp.sum(expd, axis=1, keepdims=True))
                p_ref[0, head, :, ROW_OFF[blk]:ROW_OFF[blk] + keys] = prob
                probs.append(bf(prob))
            context = nn(jnp.concatenate(probs, axis=1), jnp.concatenate([v_heads[0][:keys], v_heads[1][:keys]], axis=0))
            ctx_ref[0, blk * BLK:(blk + 1) * BLK, lanes] = bf(context)
    x1_ref[0] = bf(x_in.astype(F32) + nn(ctx_ref[0], w_ref[3 * INNER:]))


def cross_mlp(begin, part_ref, pack_ref, mlp_ref, gain_ref, x1_ref, enc_ref, dy_ref, *refs):
    if not begin:
        mlp_in_ref, gain_in_ref, _, *refs = refs
    y_ref, yfull_ref, dmid_ref, q_ref, kv_ref, p_ref, ctx_ref, dmlp_ref, dgain_ref, w_ref, hid_ref, dpre_ref = refs

    @pl.when(pl.program_id(0) == 0)
    def _():
        unpack(pack_ref, w_ref)
        dmlp_ref[...] = jnp.zeros_like(dmlp_ref) if begin else mlp_in_ref[...]
        dgain_ref[...] = jnp.zeros_like(dgain_ref) if begin else gain_in_ref[...]

    low, high, _ = half_masks()
    unit_act, _ = unit_norm(x1_ref[0])
    normed = bf(unit_act * gain_ref[1:2, :])
    q_ref[0] = bf(nt(normed, w_ref[:INNER]))
    kv_ref[0] = bf(nt(enc_ref[0], w_ref[INNER:3 * INNER]))
    for pair in range(PAIRS):
        lanes = pl.ds(pair * BLK, BLK)
        q_pair = q_ref[0, :, lanes]
        k_pair = kv_ref[0, :, lanes]
        v_pair = kv_ref[0, :, pl.ds(INNER + pair * BLK, BLK)]
        k_heads = (k_pair * low, k_pair * high)
        probs = []
        for sub in range(2):
            logits = rounded(nt(k_heads[sub], q_pair))
            expd = jnp.exp(logits - jnp.max(logits, axis=0, keepdims=True))
            prob = expd * (1.0 / jnp.sum(expd, axis=0, keepdims=True))
            p_ref[0, 2 * pair + sub] = prob
            probs.append(bf(prob))
        context = tn(jnp.concatenate(probs, axis=0), jnp.concatenate([v_pair * low, v_pair * high], axis=0))
        ctx_ref[0, :, lanes] = bf(context)
    mid_2 = rounded(x1_ref[0].astype(F32) + nn(ctx_ref[0], w_ref[3 * INNER:]))

    unit_3, inv_3 = unit_norm(mid_2)
    gain_3 = gain_ref[2:3, :]
    normed_3 = bf(unit_3 * gain_3)
    dy = dy_ref[0]
    out = mid_2
    d_norm = jnp.zeros((T, D), F32)
    for half in range(2):
        wi_0, wi_1, wo_t = [jnp.concatenate([mlp_ref[4 * half + row, mat * BLK:(mat + 1) * BLK] for row in range(4)], axis=0) for mat in range(3)]
        pre_0 = rounded(nn(normed_3, wi_0))
        pre_1 = rounded(nn(normed_3, wi_1))
        d_hid = rounded(nn(dy, wo_t))
        sq = pre_0 * pre_0
        tanh = jnp.tanh(GELU_C * (pre_0 + 0.044715 * (sq * pre_0)))
        cdf = 0.5 * (1.0 + tanh)
        gelu = pre_0 * cdf
        slope = cdf + (0.5 * pre_0) * (1.0 - tanh * tanh) * (GELU_C * (1.0 + (3.0 * 0.044715) * sq))
        hid_ref[...] = bf(gelu * pre_1)
        dpre_ref[:, 0:512] = bf((d_hid * pre_1) * slope)
        dpre_ref[:, 512:1024] = bf(d_hid * gelu)
        out = out + nt(hid_ref[...], wo_t)
        d_norm = d_norm + nt(dpre_ref[:, 0:512], wi_0) + nt(dpre_ref[:, 512:1024], wi_1)
        grad_in = tn(normed_3, dpre_ref[...])
        grad_out = tn(dy, hid_ref[...])
        for row in range(4):
            rows = slice(row * BLK, (row + 1) * BLK)
            dmlp_ref[4 * half + row, 0:BLK] += grad_in[rows, 0:512]
            dmlp_ref[4 * half + row, BLK:2 * BLK] += grad_in[rows, 512:1024]
            dmlp_ref[4 * half + row, 2 * BLK:3 * BLK] += grad_out[rows]
    y_ref[0] = bf(out)
    yfull_ref[0] = y_ref[0]
    d_act, d_gain = norm_back(d_norm, unit_3, inv_3, gain_3)
    dgain_ref[...] += jnp.broadcast_to(d_gain, (8, D))
    dmid_ref[0] = bf(dy.astype(F32) + d_act)


def cross_bwd(begin, part_ref, pack_ref, gain_ref, x1_ref, enc_ref, dmid_ref, q_ref, kv_ref, p_ref, ctx_ref, *refs):
    if not begin:
        dw_in_ref, gain_in_ref, _, *refs = refs
    dx1_ref, denc_ref, dencfull_ref, dw_ref, dgain_ref, w_ref, acc_ref, dq_ref, dkv_ref, dctx_ref = refs
    step = pl.program_id(0)

    @pl.when(step == 0)
    def _():
        unpack(pack_ref, w_ref)
        if begin:
            acc_ref[...] = jnp.zeros_like(acc_ref)
        else:
            unpack(dw_in_ref, acc_ref)
        dgain_ref[...] = jnp.zeros_like(dgain_ref) if begin else gain_in_ref[...]

    low, high, _ = half_masks()
    d_mid = dmid_ref[0]
    dctx_ref[...] = bf(nt(d_mid, w_ref[3 * INNER:]))
    acc_ref[3 * INNER:] += tn(ctx_ref[0], d_mid)
    for pair in range(PAIRS):
        lanes = pl.ds(pair * BLK, BLK)
        q_pair = q_ref[0, :, lanes]
        k_pair = kv_ref[0, :, lanes]
        v_pair = kv_ref[0, :, pl.ds(INNER + pair * BLK, BLK)]
        dctx_pair = dctx_ref[:, lanes]
        v_heads = (v_pair * low, v_pair * high)
        probs, d_logits = [], []
        for sub in range(2):
            prob = p_ref[0, 2 * pair + sub]
            d_prob = rounded(nt(v_heads[sub], dctx_pair))
            delta = jnp.sum(prob * d_prob, axis=0, keepdims=True)
            d_logits.append(bf(prob * (d_prob - delta)))
            probs.append(bf(prob))
        d_logit = jnp.concatenate(d_logits, axis=0)
        dq_ref[:, lanes] = bf(tn(d_logit, jnp.concatenate([k_pair * low, k_pair * high], axis=0)))
        dk_both = nn(d_logit, q_pair)
        dkv_ref[:, lanes] = bf(pick_half(dk_both[:E], dk_both[E:]))
        dv_both = nn(jnp.concatenate(probs, axis=0), dctx_pair)
        dkv_ref[:, pl.ds(INNER + pair * BLK, BLK)] = bf(pick_half(dv_both[:E], dv_both[E:]))
    denc_ref[0] = bf(nn(dkv_ref[...], w_ref[INNER:3 * INNER]))
    dencfull_ref[0] = denc_ref[0]
    acc_ref[INNER:3 * INNER] += tn(dkv_ref[...], enc_ref[0])
    unit_act, inv_rms = unit_norm(x1_ref[0])
    gain = gain_ref[1:2, :]
    acc_ref[:INNER] += tn(dq_ref[...], bf(unit_act * gain))
    d_act, d_gain = norm_back(nn(dq_ref[...], w_ref[:INNER]), unit_act, inv_rms, gain)
    dgain_ref[...] += jnp.broadcast_to(d_gain, (8, D))
    dx1_ref[0] = bf(d_mid.astype(F32) + d_act)

    @pl.when(step == pl.num_programs(0) - 1)
    def _():
        repack(acc_ref, dw_ref)


def self_bwd(begin, part_ref, pack_ref, gain_ref, x_ref, dmid_ref, qkv_ref, p_ref, ctx_ref, *refs):
    if not begin:
        dw_in_ref, gain_in_ref, bias_in_ref, _, *refs = refs
    dx_ref, dxfull_ref, dw_ref, dgain_ref, dbias_ref, w_ref, acc_ref, dqkv_ref, dctx_ref = refs
    step = pl.program_id(0)

    @pl.when(step == 0)
    def _():
        unpack(pack_ref, w_ref)
        if begin:
            acc_ref[...] = jnp.zeros_like(acc_ref)
        else:
            unpack(dw_in_ref, acc_ref)
        dgain_ref[...] = jnp.zeros_like(dgain_ref) if begin else gain_in_ref[...]
        dbias_ref[...] = jnp.zeros_like(dbias_ref) if begin else bias_in_ref[...]

    low, high, _ = half_masks()
    d_mid = dmid_ref[0]
    dctx_ref[...] = bf(nt(d_mid, w_ref[3 * INNER:]))
    acc_ref[3 * INNER:] += tn(ctx_ref[0], d_mid)
    for pair in range(PAIRS):
        q_pair = qkv_ref[0, :, pl.ds(pair * BLK, BLK)]
        k_pair = qkv_ref[0, :, pl.ds(INNER + pair * BLK, BLK)]
        v_pair = qkv_ref[0, :, pl.ds(2 * INNER + pair * BLK, BLK)]
        dctx_pair = dctx_ref[:, pl.ds(pair * BLK, BLK)]
        k_heads = (k_pair * low, k_pair * high)
        v_heads = (v_pair * low, v_pair * high)
        probs, d_logits = [[], []], [[], []]
        for blk in range(3):
            keys = (blk + 1) * BLK
            for sub in range(2):
                head = 2 * pair + sub
                prob = p_ref[0, head, :, ROW_OFF[blk]:ROW_OFF[blk] + keys]
                d_prob = rounded(nt(dctx_pair[blk * BLK:(blk + 1) * BLK], v_heads[sub][:keys]))
                delta = jnp.sum(prob * d_prob, axis=1, keepdims=True)
                d_logit = prob * (d_prob - delta)
                for key_blk in range(blk + 1):
                    dbias_ref[head, blk - key_blk] += d_logit[:, key_blk * BLK:(key_blk + 1) * BLK]
                d_logits[sub].append(bf(d_logit))
                probs[sub].append(bf(prob))
            d_query = nn(jnp.concatenate([d_logits[0][blk], d_logits[1][blk]], axis=1),
                         jnp.concatenate([k_heads[0][:keys], k_heads[1][:keys]], axis=0))
            dqkv_ref[blk * BLK:(blk + 1) * BLK, pl.ds(pair * BLK, BLK)] = bf(d_query)
        for vals, rhs, base in ((d_logits, q_pair, INNER), (probs, dctx_pair, 2 * INNER)):
            for key_blk in range(3):
                cols = slice(key_blk * BLK, (key_blk + 1) * BLK)
                left = jnp.concatenate([jnp.concatenate([vals[sub][blk][:, cols] for blk in range(key_blk, 3)], axis=0) for sub in range(2)], axis=1)
                both = tn(left, rhs[key_blk * BLK:])
                dqkv_ref[cols, pl.ds(base + pair * BLK, BLK)] = bf(pick_half(both[:BLK], both[BLK:]))
    unit_act, inv_rms = unit_norm(x_ref[0])
    gain = gain_ref[0:1, :]
    acc_ref[:3 * INNER] += tn(dqkv_ref[...], bf(unit_act * gain))
    d_act, d_gain = norm_back(nn(dqkv_ref[...], w_ref[:3 * INNER]), unit_act, inv_rms, gain)
    dgain_ref[...] += jnp.broadcast_to(d_gain, (8, D))
    dx_ref[0] = bf(d_mid.astype(F32) + d_act)
    dxfull_ref[0] = dx_ref[0]

    @pl.when(step == pl.num_programs(0) - 1)
    def _():
        repack(acc_ref, dw_ref)


def bucket_sums(dbias_ref, dg1_ref, dg2_ref, dg3_ref, out_ref):
    blocks = [bucket_block(diag) for diag in range(3)]
    buckets = [jnp.where(rel >= 0, bucket, -1) for rel, bucket in blocks]

    lane = lax.broadcasted_iota(jnp.int32, (8, BLK), 1)

    def one_bucket(bucket_no, sums):
        rows = []
        for head in range(6):
            total = jnp.zeros((BLK, BLK), F32)
            for diag in range(3):
                total = total + jnp.where(buckets[diag] == bucket_no, dbias_ref[head, diag], 0.0)
            rows.append(jnp.sum(total, axis=0, keepdims=True))
        rows += [jnp.zeros((1, BLK), F32)] * 2
        per_head = jnp.sum(jnp.concatenate(rows, axis=0), axis=1, keepdims=True)
        return jnp.where(lane == bucket_no, per_head, sums)

    out_ref[:, D:] = lax.fori_loop(0, NUM_BUCKETS, one_bucket, jnp.zeros((8, BLK), F32))
    row = lax.broadcasted_iota(jnp.int32, (8, D), 0)
    out_ref[:, :D] = jnp.where(row == 0, dg1_ref[...], jnp.where(row == 1, dg2_ref[...], dg3_ref[...]))


def seq_block(first, *dims):
    zeros = (0,) * len(dims)
    return pl.BlockSpec((1,) + dims, lambda i, part: (first + i,) + zeros)


def arg_block(first, *dims):
    zeros = (0,) * len(dims)
    return pl.BlockSpec((1,) + dims, lambda i, part: (part[0] * 8 + first + i,) + zeros)


def whole(*dims):
    zeros = (0,) * len(dims)
    return pl.BlockSpec(dims, lambda i, part: zeros)


def shape(dims, dtype):
    return jax.ShapeDtypeStruct(dims, dtype)


def whole_out(dims, dtype):
    return whole(*dims), shape(dims, dtype)


def call(body, seqs, flops, in_specs, outs, scratch, args, aliases=None):
    out_specs, out_shape = zip(*outs)
    return pl.pallas_call(
        body,
        out_shape=out_shape,
        grid_spec=pltpu.PrefetchScalarGridSpec(num_scalar_prefetch=1, grid=(seqs,), in_specs=in_specs, out_specs=out_specs, scratch_shapes=scratch),
        input_output_aliases=aliases or {},
        compiler_params=pltpu.CompilerParams(dimension_semantics=("arbitrary",), vmem_limit_bytes=VMEM_LIMIT),
        cost_estimate=pl.CostEstimate(flops=flops * seqs, bytes_accessed=5_000_000 * seqs, transcendentals=0),
    )(*args)


def layer_shard(dec_in, enc_out, grad_out, rel_bias, self_q, self_k, self_v, self_o, cross_q, cross_k, cross_v, cross_o, mlp_wi_0, mlp_wi_1, mlp_wo, norm_self, norm_cross, norm_mlp):
    axes = ("model", "data")
    batch = dec_in.shape[0]
    seqs = batch // 2
    chunk = seqs // 2
    part = lax.axis_index("model").astype(jnp.int32).reshape(1)
    rows = (norm_self[None], norm_cross[None], norm_mlp[None], jnp.pad(rel_bias.T, ((0, 0), (0, BLK - NUM_BUCKETS))))
    small = sum(jnp.pad(val, ((pos, 16 - pos - val.shape[0]), (0, 0))) for pos, val in enumerate(rows))
    small = lax.all_gather(small, axes).astype(F32)
    gains = small[:4].transpose(1, 0, 2).reshape(16, D)[:8]
    table = small[:, 3:6].reshape(2, 4, 3, BLK)[:, 0].reshape(6, BLK)
    table = jnp.pad(table, ((0, 2), (0, 0)))
    w_self = lax.all_gather(jnp.concatenate([self_q.T, self_k.T, self_v.T, self_o], axis=0), axes)
    w_cross = lax.all_gather(jnp.concatenate([cross_q.T, cross_k.T, cross_v.T, cross_o], axis=0), axes)
    w_mlp = lax.all_gather(jnp.concatenate([mlp_wi_0, mlp_wi_1, mlp_wo.T], axis=0), axes)

    vmem = pltpu.VMEM
    pack_spec = whole(8, 768, BLK)
    any_spec = pl.BlockSpec(memory_space=pl.ANY)
    w_scr = vmem((1536, D), BF)
    acc_scr = vmem((1536, D), F32)
    full_out = {rows: shape((batch, rows, D), BF) for rows in (T, E)}
    model_no = lax.axis_index("model")

    def seq_out(count, dims, dtype):
        return seq_block(0, *dims), shape((count,) + dims, dtype)

    def send(val):
        return lax.ppermute(val, "model", [(0, 1), (1, 0)])

    def scatter(val):
        return lax.psum_scatter(val, axes, scatter_dimension=0)

    def place(full, received):
        for pos, val in enumerate(received):
            full = lax.dynamic_update_slice(full, val, ((1 - model_no) * seqs + pos * chunk, 0, 0))
        return full

    mid_1, qkv, probs, ctx = call(
        self_fwd, seqs, 7_000_000_000,
        [pack_spec, whole(8, D), whole(8, BLK), arg_block(0, T, D)],
        [seq_out(seqs, (T, D), BF), seq_out(seqs, (T, 3 * INNER), BF), seq_out(seqs, (6, BLK, 768), F32), seq_out(seqs, (T, INNER), BF)],
        [w_scr, vmem((6, 3, BLK, BLK), F32)],
        (part, w_self, gains, table, dec_in))

    saved, got_y, chain = [], [], ()
    for pos in range(2):
        first = pos * chunk
        extra = [whole(8, 384, D), whole(8, D), any_spec] if pos else []
        y_part, y_full, d_mid, q_x, kv_x, probs_x, ctx_x, d_mlp, d_gain_3 = call(
            functools.partial(cross_mlp, pos == 0), chunk, 14_000_000_000,
            [pack_spec, whole(8, 384, D), whole(8, D), seq_block(first, T, D), arg_block(first, E, D), arg_block(first, T, D)] + extra,
            [seq_out(chunk, (T, D), BF), (arg_block(first, T, D), full_out[T]), seq_out(chunk, (T, D), BF), seq_out(chunk, (T, INNER), BF), seq_out(chunk, (E, 2 * INNER), BF),
             seq_out(chunk, (6, E, T), F32), seq_out(chunk, (T, INNER), BF), whole_out((8, 384, D), F32), whole_out((8, D), F32)],
            [w_scr, vmem((T, 512), BF), vmem((T, 1024), BF)],
            (part, w_cross, w_mlp, gains, mid_1, enc_out, grad_out) + chain, {9: 1} if pos else None)
        chain = (d_mlp, d_gain_3, y_full)
        got_y.append(send(y_part))
        saved.append((d_mid, q_x, kv_x, probs_x, ctx_x))
    d_mlp = scatter(d_mlp)

    d_mids, got_e, chain = [], [], ()
    for pos in range(2):
        first = pos * chunk
        extra = [pack_spec, whole(8, D), any_spec] if pos else []
        d_mid_1, e_part, e_full, d_cross, d_gain_2 = call(
            functools.partial(cross_bwd, pos == 0), chunk, 7_000_000_000,
            [pack_spec, whole(8, D), seq_block(first, T, D), arg_block(first, E, D), seq_block(0, T, D), seq_block(0, T, INNER), seq_block(0, E, 2 * INNER), seq_block(0, 6, E, T), seq_block(0, T, INNER)] + extra,
            [seq_out(chunk, (T, D), BF), seq_out(chunk, (E, D), BF), (arg_block(first, E, D), full_out[E]), whole_out((8, 768, BLK), F32), whole_out((8, D), F32)],
            [w_scr, acc_scr, vmem((T, INNER), BF), vmem((E, 2 * INNER), BF), vmem((T, INNER), BF)],
            (part, w_cross, gains, mid_1, enc_out) + saved[pos] + chain, {12: 2} if pos else None)
        chain = (d_cross, d_gain_2, e_full)
        got_e.append(send(e_part))
        d_mids.append(d_mid_1)
    d_cross = scatter(d_cross)

    got_x, chain = [], ()
    for pos in range(2):
        first = pos * chunk
        extra = [pack_spec, whole(8, D), whole(6, 3, BLK, BLK), any_spec] if pos else []
        x_part, x_full, d_self, d_gain_1, d_bias = call(
            functools.partial(self_bwd, pos == 0), chunk, 11_000_000_000,
            [pack_spec, whole(8, D), arg_block(first, T, D), seq_block(0, T, D), seq_block(first, T, 3 * INNER), seq_block(first, 6, BLK, 768), seq_block(first, T, INNER)] + extra,
            [seq_out(chunk, (T, D), BF), (arg_block(first, T, D), full_out[T]), whole_out((8, 768, BLK), F32), whole_out((8, D), F32), whole_out((6, 3, BLK, BLK), F32)],
            [w_scr, acc_scr, vmem((T, 3 * INNER), BF), vmem((T, INNER), BF)],
            (part, w_self, gains, dec_in, d_mids[pos], qkv, probs, ctx) + chain, {11: 1} if pos else None)
        chain = (d_self, d_gain_1, d_bias, x_full)
        got_x.append(send(x_part))
    d_self = scatter(d_self)

    tiny = pl.pallas_call(bucket_sums, name="bucket_sums", out_shape=shape((8, D + BLK), F32))(d_bias, d_gain_1, d_gain_2, d_gain_3)
    tiny = lax.psum(tiny, axes)
    data_no = lax.axis_index("data")
    gain_grads = lax.dynamic_slice(tiny, (0, data_no * BLK), (3, BLK))
    gain_grads = (gain_grads[0], gain_grads[1], gain_grads[2])
    bias_sums = tiny[:, D:D + NUM_BUCKETS]
    grad_bias = jnp.where(model_no == 0, bias_sums[0:3], bias_sums[3:6]).T

    dec_out, grad_enc, grad_dec = place(y_full, got_y), place(e_full, got_e), place(x_full, got_x)

    def split_attn(grad_pack):
        mats = [grad_pack[192 * pos:192 * (pos + 1)] for pos in range(4)]
        return mats[0].T, mats[1].T, mats[2].T, mats[3]

    return (dec_out, grad_dec, grad_enc, grad_bias) + split_attn(d_self) + split_attn(d_cross) + (
        d_mlp[:BLK], d_mlp[BLK:2 * BLK], d_mlp[2 * BLK:].T) + gain_grads


def solution(mesh):
    row_spec = P("data", None, None)
    col_in = P("data", "model")
    col_out = P("model", "data")
    gain_spec = P("data")
    bias_spec = P(None, "model")
    arg_specs = (row_spec, row_spec, row_spec, bias_spec, col_in, col_in, col_in, col_out, col_in, col_in, col_in, col_out, col_in, col_in, col_out, gain_spec, gain_spec, gain_spec)
    out_specs = (row_spec, row_spec, row_spec) + arg_specs[3:]

    return jax.shard_map(layer_shard, mesh=mesh, in_specs=arg_specs, out_specs=out_specs, check_vma=False)
```

```python
import functools
import math
import jax
import jax.numpy as jnp
import numpy as np
from jax import lax
from jax.experimental import pallas as pl
from jax.experimental.pallas import tpu as pltpu
from jax.sharding import PartitionSpec as P

EPS = 1e-6
BUCKET_EDGES = tuple(math.ceil(16 * 8.0 ** (bucket_no / 16.0)) for bucket_no in range(1, 16))
NUM_BUCKETS = 32
D, INNER = 512, 384
T, E = 384, 192
PAIRS, BLK = 3, 128
ROWS = 1568
ROW_OFF = (0, 128, 384)
F32, BF = jnp.float32, jnp.bfloat16
GELU_C = math.sqrt(2.0 / math.pi)
VMEM_LIMIT = 60 * 1024 * 1024


def nn(lhs, rhs):
    return lax.dot_general(lhs, rhs, (((1,), (0,)), ((), ())), preferred_element_type=F32)


def nt(lhs, rhs):
    return lax.dot_general(lhs, rhs, (((1,), (1,)), ((), ())), preferred_element_type=F32)


def tn(lhs, rhs):
    return lax.dot_general(lhs, rhs, (((0,), (0,)), ((), ())), preferred_element_type=F32)


def bf(val):
    return val.astype(BF)


def rounded(val):
    return val.astype(BF).astype(F32)


def unit_norm(act):
    act_f = act.astype(F32)
    inv_rms = lax.rsqrt(jnp.mean(act_f * act_f, axis=-1, keepdims=True) + EPS)
    return act_f * inv_rms, inv_rms


def norm_back(d_norm, unit_act, inv_rms, gain):
    d_norm_f = rounded(d_norm)
    d_unit = d_norm_f * gain
    d_act = inv_rms * (d_unit - unit_act * jnp.mean(d_unit * unit_act, axis=-1, keepdims=True))
    return d_act, jnp.sum(d_norm_f * unit_act, axis=0, keepdims=True)


def gain_rows(small_ref):
    return jnp.concatenate([small_ref[row] for row in range(4)], axis=1).astype(F32)


def half_masks():
    lane = lax.broadcasted_iota(jnp.int32, (1, BLK), 1)
    low = jnp.where(lane < 64, 1.0, 0.0)
    return bf(low), bf(1.0 - low), lane < 64


def pick_half(low_rows, high_rows):
    lane = lax.broadcasted_iota(jnp.int32, low_rows.shape, 1)
    return jnp.where(lane < 64, low_rows, high_rows)


def pack_slots():
    for row in range(4):
        for half in range(2):
            for mat in range(4):
                first = mat * INNER + half * 192
                yield 4 * half + row, slice(mat * 192, (mat + 1) * 192), slice(first, first + 192), slice(row * BLK, (row + 1) * BLK)


def unpack(pack_ref, full_ref):
    for dev, rows, feats, cols in pack_slots():
        full_ref[feats, cols] = pack_ref[dev, rows, :]


def repack(full_ref, pack_ref):
    for dev, rows, feats, cols in pack_slots():
        pack_ref[dev, rows, :] = full_ref[feats, cols]


def bucket_block(diag):
    row = lax.broadcasted_iota(jnp.int32, (BLK, BLK), 0)
    col = lax.broadcasted_iota(jnp.int32, (BLK, BLK), 1)
    rel = row - col + diag * BLK
    bucket = jnp.clip(rel, 0, 16)
    for edge in BUCKET_EDGES:
        bucket = bucket + jnp.where(rel >= edge, 1, 0)
    return rel, bucket


def build_bias(small_ref, bias_ref):
    tables = [small_ref[0].astype(F32), small_ref[4].astype(F32)]
    for diag in range(3):
        rel, bucket = bucket_block(diag)
        for head in range(6):
            pos = 3 + head % 3
            row = jnp.broadcast_to(tables[head // 3][pos:pos + 1, :], (BLK, BLK))
            vals = jnp.take_along_axis(row, bucket, axis=1, mode="promise_in_bounds")
            bias_ref[head, diag] = jnp.where(rel >= 0, vals, -jnp.inf)


def self_fwd(part_ref, pack_ref, small_ref, x_ref, x1_ref, qkv_ref, p_ref, ctx_ref, w_ref, bias_ref):
    @pl.when(pl.program_id(0) == 0)
    def _():
        unpack(pack_ref, w_ref)
        build_bias(small_ref, bias_ref)

    low, high, _ = half_masks()
    x_in = x_ref[0]
    unit_act, _ = unit_norm(x_in)
    normed = bf(unit_act * gain_rows(small_ref)[0:1])
    qkv_ref[0] = bf(nt(normed, w_ref[:3 * INNER]))
    for pair in range(PAIRS):
        lanes = pl.ds(pair * BLK, BLK)
        q_pair = qkv_ref[0, :, pl.ds(pair * BLK, BLK)]
        k_pair = qkv_ref[0, :, pl.ds(INNER + pair * BLK, BLK)]
        v_pair = qkv_ref[0, :, pl.ds(2 * INNER + pair * BLK, BLK)]
        k_heads = (k_pair * low, k_pair * high)
        v_heads = (v_pair * low, v_pair * high)
        for blk in range(3):
            keys = (blk + 1) * BLK
            q_rows = q_pair[blk * BLK:(blk + 1) * BLK]
            probs = []
            for sub in range(2):
                head = 2 * pair + sub
                bias = jnp.concatenate([bias_ref[head, blk - key_blk] for key_blk in range(blk + 1)], axis=1)
                logits = rounded(nt(q_rows, k_heads[sub][:keys])) + bias
                expd = jnp.exp(logits - jnp.max(logits, axis=1, keepdims=True))
                prob = expd * (1.0 / jnp.sum(expd, axis=1, keepdims=True))
                p_ref[0, head, :, ROW_OFF[blk]:ROW_OFF[blk] + keys] = prob
                probs.append(bf(prob))
            context = nn(jnp.concatenate(probs, axis=1), jnp.concatenate([v_heads[0][:keys], v_heads[1][:keys]], axis=0))
            ctx_ref[0, blk * BLK:(blk + 1) * BLK, lanes] = bf(context)
    x1_ref[0] = bf(x_in.astype(F32) + nn(ctx_ref[0], w_ref[3 * INNER:]))


def cross_mlp(begin, part_ref, pack_ref, small_ref, x1_ref, enc_ref, dy_ref, *refs):
    if not begin:
        mlp_in_ref, gain_in_ref, _, *refs = refs
    y_ref, yfull_ref, dmid_ref, q_ref, kv_ref, p_ref, ctx_ref, dmlp_ref, dgain_ref, w_ref, mlp_ref, hid_ref, dpre_ref = refs

    @pl.when(pl.program_id(0) == 0)
    def _():
        unpack(pack_ref, w_ref)
        for half, mat, row, blk in np.ndindex(2, 2, 4, 4):
            first = 768 + 512 * mat + BLK * blk
            mlp_ref[half, mat, row * BLK:(row + 1) * BLK, blk * BLK:(blk + 1) * BLK] = pack_ref[4 * half + row, first:first + BLK, :]
        for half, row in np.ndindex(2, 4):
            mlp_ref[half, 2, :, row * BLK:(row + 1) * BLK] = pack_ref[4 * half + row, 1792:2304, :]
        dmlp_ref[...] = jnp.zeros_like(dmlp_ref) if begin else mlp_in_ref[...]
        dgain_ref[...] = jnp.zeros_like(dgain_ref) if begin else gain_in_ref[...]

    low, high, _ = half_masks()
    unit_act, _ = unit_norm(x1_ref[0])
    gains = gain_rows(small_ref)
    normed = bf(unit_act * gains[1:2])
    q_ref[0] = bf(nt(normed, w_ref[:INNER]))
    kv_ref[0] = bf(nt(enc_ref[0], w_ref[INNER:3 * INNER]))
    for pair in range(PAIRS):
        lanes = pl.ds(pair * BLK, BLK)
        q_pair = q_ref[0, :, lanes]
        k_pair = kv_ref[0, :, lanes]
        v_pair = kv_ref[0, :, pl.ds(INNER + pair * BLK, BLK)]
        k_heads = (k_pair * low, k_pair * high)
        probs = []
        for sub in range(2):
            logits = rounded(nt(k_heads[sub], q_pair))
            expd = jnp.exp(logits - jnp.max(logits, axis=0, keepdims=True))
            prob = expd * (1.0 / jnp.sum(expd, axis=0, keepdims=True))
            p_ref[0, 2 * pair + sub] = prob
            probs.append(bf(prob))
        context = tn(jnp.concatenate(probs, axis=0), jnp.concatenate([v_pair * low, v_pair * high], axis=0))
        ctx_ref[0, :, lanes] = bf(context)
    mid_2 = rounded(x1_ref[0].astype(F32) + nn(ctx_ref[0], w_ref[3 * INNER:]))

    unit_3, inv_3 = unit_norm(mid_2)
    gain_3 = gains[2:3]
    normed_3 = bf(unit_3 * gain_3)
    dy = dy_ref[0]
    out = mid_2
    d_norm = jnp.zeros((T, D), F32)
    for half in range(2):
        wi_0, wi_1, w_out = mlp_ref[half, 0], mlp_ref[half, 1], mlp_ref[half, 2]
        pre_0 = rounded(nn(normed_3, wi_0))
        pre_1 = rounded(nn(normed_3, wi_1))
        d_hid = rounded(nt(dy, w_out))
        sq = pre_0 * pre_0
        tanh = jnp.tanh(GELU_C * (pre_0 + 0.044715 * (sq * pre_0)))
        cdf = 0.5 * (1.0 + tanh)
        gelu = pre_0 * cdf
        slope = cdf + (0.5 * pre_0) * (1.0 - tanh * tanh) * (GELU_C * (1.0 + (3.0 * 0.044715) * sq))
        hid_ref[...] = bf(gelu * pre_1)
        dpre_ref[:, 0:512] = bf((d_hid * pre_1) * slope)
        dpre_ref[:, 512:1024] = bf(d_hid * gelu)
        out = out + nn(hid_ref[...], w_out)
        d_norm = d_norm + nt(dpre_ref[:, 0:512], wi_0) + nt(dpre_ref[:, 512:1024], wi_1)
        grad_in = tn(normed_3, dpre_ref[...])
        grad_out = tn(hid_ref[...], dy)
        for row in range(4):
            rows = slice(row * BLK, (row + 1) * BLK)
            for blk in range(8):
                cols = slice(blk * BLK, (blk + 1) * BLK)
                dmlp_ref[4 * half + row, cols, :] += grad_in[rows, cols]
            dmlp_ref[4 * half + row, 1024:1536, :] += grad_out[:, rows]
    y_ref[0] = bf(out)
    yfull_ref[0] = y_ref[0]
    d_act, d_gain = norm_back(d_norm, unit_3, inv_3, gain_3)
    dgain_ref[...] += jnp.broadcast_to(d_gain, (8, D))
    dmid_ref[0] = bf(dy.astype(F32) + d_act)


def cross_bwd(begin, part_ref, pack_ref, small_ref, x1_ref, enc_ref, dmid_ref, q_ref, kv_ref, p_ref, ctx_ref, *refs):
    if not begin:
        dw_in_ref, gain_in_ref, _, *refs = refs
    dx1_ref, denc_ref, dencfull_ref, dw_ref, dgain_ref, w_ref, acc_ref, dq_ref, dkv_ref, dctx_ref = refs
    step = pl.program_id(0)

    @pl.when(step == 0)
    def _():
        unpack(pack_ref, w_ref)
        if begin:
            acc_ref[...] = jnp.zeros_like(acc_ref)
        else:
            unpack(dw_in_ref, acc_ref)
        dgain_ref[...] = jnp.zeros_like(dgain_ref) if begin else gain_in_ref[...]

    low, high, _ = half_masks()
    d_mid = dmid_ref[0]
    dctx_ref[...] = bf(nt(d_mid, w_ref[3 * INNER:]))
    acc_ref[3 * INNER:] += tn(ctx_ref[0], d_mid)
    for pair in range(PAIRS):
        lanes = pl.ds(pair * BLK, BLK)
        q_pair = q_ref[0, :, lanes]
        k_pair = kv_ref[0, :, lanes]
        v_pair = kv_ref[0, :, pl.ds(INNER + pair * BLK, BLK)]
        dctx_pair = dctx_ref[:, lanes]
        v_heads = (v_pair * low, v_pair * high)
        probs, d_logits = [], []
        for sub in range(2):
            prob = p_ref[0, 2 * pair + sub]
            d_prob = rounded(nt(v_heads[sub], dctx_pair))
            delta = jnp.sum(prob * d_prob, axis=0, keepdims=True)
            d_logits.append(bf(prob * (d_prob - delta)))
            probs.append(bf(prob))
        d_logit = jnp.concatenate(d_logits, axis=0)
        dq_ref[:, lanes] = bf(tn(d_logit, jnp.concatenate([k_pair * low, k_pair * high], axis=0)))
        dk_both = nn(d_logit, q_pair)
        dkv_ref[:, lanes] = bf(pick_half(dk_both[:E], dk_both[E:]))
        dv_both = nn(jnp.concatenate(probs, axis=0), dctx_pair)
        dkv_ref[:, pl.ds(INNER + pair * BLK, BLK)] = bf(pick_half(dv_both[:E], dv_both[E:]))
    denc_ref[0] = bf(nn(dkv_ref[...], w_ref[INNER:3 * INNER]))
    dencfull_ref[0] = denc_ref[0]
    acc_ref[INNER:3 * INNER] += tn(dkv_ref[...], enc_ref[0])
    unit_act, inv_rms = unit_norm(x1_ref[0])
    gain = gain_rows(small_ref)[1:2]
    acc_ref[:INNER] += tn(dq_ref[...], bf(unit_act * gain))
    d_act, d_gain = norm_back(nn(dq_ref[...], w_ref[:INNER]), unit_act, inv_rms, gain)
    dgain_ref[...] += jnp.broadcast_to(d_gain, (8, D))
    dx1_ref[0] = bf(d_mid.astype(F32) + d_act)

    @pl.when(step == pl.num_programs(0) - 1)
    def _():
        repack(acc_ref, dw_ref)


def add_small(dg1_ref, dg2_ref, dg3_ref, dbias_ref, dw_ref):
    blocks = [bucket_block(diag) for diag in range(3)]
    buckets = [jnp.where(rel >= 0, bucket, -1) for rel, bucket in blocks]
    lane = lax.broadcasted_iota(jnp.int32, (8, BLK), 1)

    def one_bucket(bucket_no, sums):
        rows = []
        for head in range(6):
            total = jnp.zeros((BLK, BLK), F32)
            for diag in range(3):
                total = total + jnp.where(buckets[diag] == bucket_no, dbias_ref[head, diag], 0.0)
            rows.append(jnp.sum(total, axis=0, keepdims=True))
        rows += [jnp.zeros((1, BLK), F32)] * 2
        per_head = jnp.sum(jnp.concatenate(rows, axis=0), axis=1, keepdims=True)
        return jnp.where(lane == bucket_no, per_head, sums)

    sums = lax.fori_loop(0, NUM_BUCKETS, one_bucket, jnp.zeros((8, BLK), F32))
    gains = [ref[...] for ref in (dg1_ref, dg2_ref, dg3_ref)]
    for half in range(2):
        for row in range(4):
            parts = [gain[0:1, row * BLK:(row + 1) * BLK] for gain in gains]
            parts += [sums[3 * half:3 * half + 3], jnp.zeros((2, BLK), F32)]
            dw_ref[4 * half + row, 1536:1544, :] = jnp.concatenate(parts, axis=0)


def self_bwd(begin, part_ref, pack_ref, small_ref, x_ref, dmid_ref, qkv_ref, p_ref, ctx_ref, *refs):
    if not begin:
        dw_in_ref, gain_in_ref, bias_in_ref, dcross_ref, dg2_ref, dg3_ref, _, *refs = refs
    dx_ref, dxfull_ref, dw_ref, dgain_ref, dbias_ref, w_ref, acc_ref, dqkv_ref, dctx_ref = refs
    step = pl.program_id(0)

    @pl.when(step == 0)
    def _():
        unpack(pack_ref, w_ref)
        if begin:
            acc_ref[...] = jnp.zeros_like(acc_ref)
        else:
            unpack(dw_in_ref, acc_ref)
        dgain_ref[...] = jnp.zeros_like(dgain_ref) if begin else gain_in_ref[...]
        dbias_ref[...] = jnp.zeros_like(dbias_ref) if begin else bias_in_ref[...]

    low, high, _ = half_masks()
    d_mid = dmid_ref[0]
    dctx_ref[...] = bf(nt(d_mid, w_ref[3 * INNER:]))
    acc_ref[3 * INNER:] += tn(ctx_ref[0], d_mid)
    for pair in range(PAIRS):
        q_pair = qkv_ref[0, :, pl.ds(pair * BLK, BLK)]
        k_pair = qkv_ref[0, :, pl.ds(INNER + pair * BLK, BLK)]
        v_pair = qkv_ref[0, :, pl.ds(2 * INNER + pair * BLK, BLK)]
        dctx_pair = dctx_ref[:, pl.ds(pair * BLK, BLK)]
        k_heads = (k_pair * low, k_pair * high)
        v_heads = (v_pair * low, v_pair * high)
        probs, d_logits = [[], []], [[], []]
        for blk in range(3):
            keys = (blk + 1) * BLK
            for sub in range(2):
                head = 2 * pair + sub
                prob = p_ref[0, head, :, ROW_OFF[blk]:ROW_OFF[blk] + keys]
                d_prob = rounded(nt(dctx_pair[blk * BLK:(blk + 1) * BLK], v_heads[sub][:keys]))
                delta = jnp.sum(prob * d_prob, axis=1, keepdims=True)
                d_logit = prob * (d_prob - delta)
                for key_blk in range(blk + 1):
                    dbias_ref[head, blk - key_blk] += d_logit[:, key_blk * BLK:(key_blk + 1) * BLK]
                d_logits[sub].append(bf(d_logit))
                probs[sub].append(bf(prob))
            d_query = nn(jnp.concatenate([d_logits[0][blk], d_logits[1][blk]], axis=1),
                         jnp.concatenate([k_heads[0][:keys], k_heads[1][:keys]], axis=0))
            dqkv_ref[blk * BLK:(blk + 1) * BLK, pl.ds(pair * BLK, BLK)] = bf(d_query)
        for vals, rhs, base in ((d_logits, q_pair, INNER), (probs, dctx_pair, 2 * INNER)):
            for key_blk in range(3):
                cols = slice(key_blk * BLK, (key_blk + 1) * BLK)
                left = jnp.concatenate([jnp.concatenate([vals[sub][blk][:, cols] for blk in range(key_blk, 3)], axis=0) for sub in range(2)], axis=1)
                both = tn(left, rhs[key_blk * BLK:])
                dqkv_ref[cols, pl.ds(base + pair * BLK, BLK)] = bf(pick_half(both[:BLK], both[BLK:]))
    unit_act, inv_rms = unit_norm(x_ref[0])
    gain = gain_rows(small_ref)[0:1]
    acc_ref[:3 * INNER] += tn(dqkv_ref[...], bf(unit_act * gain))
    d_act, d_gain = norm_back(nn(dqkv_ref[...], w_ref[:3 * INNER]), unit_act, inv_rms, gain)
    dgain_ref[...] += jnp.broadcast_to(d_gain, (8, D))
    dx_ref[0] = bf(d_mid.astype(F32) + d_act)
    dxfull_ref[0] = dx_ref[0]

    @pl.when(step == pl.num_programs(0) - 1)
    def _():
        repack(acc_ref, dw_ref)
        if not begin:
            dw_ref[:, 768:1536, :] = dcross_ref[...]
            dw_ref[:, 1544:ROWS, :] = jnp.zeros((8, ROWS - 1544, BLK), F32)
            add_small(dgain_ref, dg2_ref, dg3_ref, dbias_ref, dw_ref)


def seq_block(first, *dims):
    zeros = (0,) * len(dims)
    return pl.BlockSpec((1,) + dims, lambda i, part: (first + i,) + zeros)


def arg_block(first, *dims):
    zeros = (0,) * len(dims)
    return pl.BlockSpec((1,) + dims, lambda i, part: (part[0] * 8 + first + i,) + zeros)


def whole(*dims):
    zeros = (0,) * len(dims)
    return pl.BlockSpec(dims, lambda i, part: zeros)


def shape(dims, dtype):
    return jax.ShapeDtypeStruct(dims, dtype)


def whole_out(dims, dtype):
    return whole(*dims), shape(dims, dtype)


def call(body, seqs, flops, in_specs, outs, scratch, args, aliases=None):
    out_specs, out_shape = zip(*outs)
    return pl.pallas_call(
        body,
        out_shape=out_shape,
        grid_spec=pltpu.PrefetchScalarGridSpec(num_scalar_prefetch=1, grid=(seqs,), in_specs=in_specs, out_specs=out_specs, scratch_shapes=scratch),
        input_output_aliases=aliases or {},
        compiler_params=pltpu.CompilerParams(dimension_semantics=("arbitrary",), vmem_limit_bytes=VMEM_LIMIT),
        cost_estimate=pl.CostEstimate(flops=flops * seqs, bytes_accessed=5_000_000 * seqs, transcendentals=0),
    )(*args)


def stack_cols(weight):
    return [weight.reshape(BLK, 4, BLK).transpose(1, 0, 2).reshape(512, BLK)]


def layer_shard(dec_in, enc_out, grad_out, rel_bias, self_q, self_k, self_v, self_o, cross_q, cross_k, cross_v, cross_o, mlp_wi_0, mlp_wi_1, mlp_wo, norm_self, norm_cross, norm_mlp):
    axes = ("model", "data")
    batch = dec_in.shape[0]
    seqs = batch // 2
    chunk = seqs // 2
    part = lax.axis_index("model").astype(jnp.int32).reshape(1)
    rows = (norm_self[None], norm_cross[None], norm_mlp[None], jnp.pad(rel_bias.T, ((0, 0), (0, BLK - NUM_BUCKETS))))
    small = sum(jnp.pad(val, ((pos, 16 - pos - val.shape[0]), (0, 0))) for pos, val in enumerate(rows))
    w_self = lax.all_gather(jnp.concatenate([self_q.T, self_k.T, self_v.T, self_o, small], axis=0), axes)
    w_rest = lax.all_gather(jnp.concatenate([cross_q.T, cross_k.T, cross_v.T, cross_o] + stack_cols(mlp_wi_0) + stack_cols(mlp_wi_1) + [mlp_wo], axis=0), axes)

    vmem = pltpu.VMEM
    pack_spec = whole(8, 768, BLK)
    small_spec = pl.BlockSpec((8, 16, BLK), lambda i, part: (0, 48, 0))
    any_spec = pl.BlockSpec(memory_space=pl.ANY)
    w_scr = vmem((1536, D), BF)
    acc_scr = vmem((1536, D), F32)
    full_out = {rows: shape((batch, rows, D), BF) for rows in (T, E)}
    model_no = lax.axis_index("model")

    def seq_out(count, dims, dtype):
        return seq_block(0, *dims), shape((count,) + dims, dtype)

    def send(val):
        return lax.ppermute(val, "model", [(0, 1), (1, 0)])

    def scatter(val):
        return lax.psum_scatter(val, axes, scatter_dimension=0)

    def place(full, received):
        for pos, val in enumerate(received):
            full = lax.dynamic_update_slice(full, val, ((1 - model_no) * seqs + pos * chunk, 0, 0))
        return full

    mid_1, qkv, probs, ctx = call(
        self_fwd, seqs, 7_000_000_000,
        [pack_spec, small_spec, arg_block(0, T, D)],
        [seq_out(seqs, (T, D), BF), seq_out(seqs, (T, 3 * INNER), BF), seq_out(seqs, (6, BLK, 768), F32), seq_out(seqs, (T, INNER), BF)],
        [w_scr, vmem((6, 3, BLK, BLK), F32)],
        (part, w_self, w_self, dec_in))

    saved, got_y, chain = [], [], ()
    for pos in range(2):
        first = pos * chunk
        extra = [whole(8, 1536, BLK), whole(8, D), any_spec] if pos else []
        y_part, y_full, d_mid, q_x, kv_x, probs_x, ctx_x, d_mlp, d_gain_3 = call(
            functools.partial(cross_mlp, pos == 0), chunk, 14_000_000_000,
            [whole(8, 2304, BLK), small_spec, seq_block(first, T, D), arg_block(first, E, D), arg_block(first, T, D)] + extra,
            [seq_out(chunk, (T, D), BF), (arg_block(first, T, D), full_out[T]), seq_out(chunk, (T, D), BF), seq_out(chunk, (T, INNER), BF), seq_out(chunk, (E, 2 * INNER), BF),
             seq_out(chunk, (6, E, T), F32), seq_out(chunk, (T, INNER), BF), whole_out((8, 1536, BLK), F32), whole_out((8, D), F32)],
            [w_scr, vmem((2, 3, 512, 512), BF), vmem((T, 512), BF), vmem((T, 1024), BF)],
            (part, w_rest, w_self, mid_1, enc_out, grad_out) + chain, {8: 1} if pos else None)
        chain = (d_mlp, d_gain_3, y_full)
        got_y.append(send(y_part))
        saved.append((d_mid, q_x, kv_x, probs_x, ctx_x))
    d_mlp = scatter(d_mlp)

    d_mids, got_e, chain = [], [], ()
    for pos in range(2):
        first = pos * chunk
        extra = [pack_spec, whole(8, D), any_spec] if pos else []
        d_mid_1, e_part, e_full, d_cross, d_gain_2 = call(
            functools.partial(cross_bwd, pos == 0), chunk, 7_000_000_000,
            [pack_spec, small_spec, seq_block(first, T, D), arg_block(first, E, D), seq_block(0, T, D), seq_block(0, T, INNER), seq_block(0, E, 2 * INNER), seq_block(0, 6, E, T), seq_block(0, T, INNER)] + extra,
            [seq_out(chunk, (T, D), BF), seq_out(chunk, (E, D), BF), (arg_block(first, E, D), full_out[E]), whole_out((8, 768, BLK), F32), whole_out((8, D), F32)],
            [w_scr, acc_scr, vmem((T, INNER), BF), vmem((E, 2 * INNER), BF), vmem((T, INNER), BF)],
            (part, w_rest, w_self, mid_1, enc_out) + saved[pos] + chain, {12: 2} if pos else None)
        chain = (d_cross, d_gain_2, e_full)
        got_e.append(send(e_part))
        d_mids.append(d_mid_1)

    got_x, chain = [], ()
    for pos in range(2):
        first = pos * chunk
        extra = [pack_spec, whole(8, D), whole(6, 3, BLK, BLK), pack_spec, whole(8, D), whole(8, D), any_spec] if pos else []
        x_part, x_full, d_self, d_gain_1, d_bias = call(
            functools.partial(self_bwd, pos == 0), chunk, 11_000_000_000,
            [pack_spec, small_spec, arg_block(first, T, D), seq_block(0, T, D), seq_block(first, T, 3 * INNER), seq_block(first, 6, BLK, 768), seq_block(first, T, INNER)] + extra,
            [seq_out(chunk, (T, D), BF), (arg_block(first, T, D), full_out[T]), whole_out((8, ROWS if pos else 768, BLK), F32), whole_out((8, D), F32), whole_out((6, 3, BLK, BLK), F32)],
            [w_scr, acc_scr, vmem((T, 3 * INNER), BF), vmem((T, INNER), BF)],
            (part, w_self, w_self, dec_in, d_mids[pos], qkv, probs, ctx) + chain, {14: 1} if pos else None)
        chain = (d_self, d_gain_1, d_bias, d_cross, d_gain_2, d_gain_3, x_full)
        got_x.append(send(x_part))
    d_self = scatter(d_self)

    gain_grads = (d_self[1536], d_self[1537], d_self[1538])
    grad_bias = d_self[1539:1542, :NUM_BUCKETS].T
    dec_out, grad_enc, grad_dec = place(y_full, got_y), place(e_full, got_e), place(x_full, got_x)

    def split_attn(grad_pack):
        mats = [grad_pack[192 * pos:192 * (pos + 1)] for pos in range(4)]
        return mats[0].T, mats[1].T, mats[2].T, mats[3]

    def join_cols(rows):
        return jnp.concatenate([rows[blk * BLK:(blk + 1) * BLK] for blk in range(4)], axis=1)

    return (dec_out, grad_dec, grad_enc, grad_bias) + split_attn(d_self) + split_attn(d_self[768:]) + (
        join_cols(d_mlp[:512]), join_cols(d_mlp[512:1024]), d_mlp[1024:]) + gain_grads


def solution(mesh):
    row_spec = P("data", None, None)
    col_in = P("data", "model")
    col_out = P("model", "data")
    gain_spec = P("data")
    bias_spec = P(None, "model")
    arg_specs = (row_spec, row_spec, row_spec, bias_spec, col_in, col_in, col_in, col_out, col_in, col_in, col_in, col_out, col_in, col_in, col_out, gain_spec, gain_spec, gain_spec)
    out_specs = (row_spec, row_spec, row_spec) + arg_specs[3:]

    return jax.shard_map(layer_shard, mesh=mesh, in_specs=arg_specs, out_specs=out_specs, check_vma=False)
```

```python
import functools
import math
import jax
import jax.numpy as jnp
import numpy as np
from jax import lax
from jax.experimental import pallas as pl
from jax.experimental.pallas import tpu as pltpu
from jax.sharding import PartitionSpec as P

EPS = 1e-6
BUCKET_EDGES = tuple(math.ceil(16 * 8.0 ** (bucket_no / 16.0)) for bucket_no in range(1, 16))
NUM_BUCKETS = 32
D, INNER = 512, 384
T, E = 384, 192
PAIRS, BLK = 3, 128
ROWS = 1568
ROW_OFF = (0, 128, 384)
F32, BF = jnp.float32, jnp.bfloat16
GELU_C = math.sqrt(2.0 / math.pi)
VMEM_LIMIT = 60 * 1024 * 1024


def nn(lhs, rhs):
    return lax.dot_general(lhs, rhs, (((1,), (0,)), ((), ())), preferred_element_type=F32)


def nt(lhs, rhs):
    return lax.dot_general(lhs, rhs, (((1,), (1,)), ((), ())), preferred_element_type=F32)


def tn(lhs, rhs):
    return lax.dot_general(lhs, rhs, (((0,), (0,)), ((), ())), preferred_element_type=F32)


def bf(val):
    return val.astype(BF)


def rounded(val):
    return val.astype(BF).astype(F32)


def unit_norm(act):
    act_f = act.astype(F32)
    inv_rms = lax.rsqrt(jnp.mean(act_f * act_f, axis=-1, keepdims=True) + EPS)
    return act_f * inv_rms, inv_rms


def norm_back(d_norm, unit_act, inv_rms, gain):
    d_norm_f = rounded(d_norm)
    d_unit = d_norm_f * gain
    d_act = inv_rms * (d_unit - unit_act * jnp.mean(d_unit * unit_act, axis=-1, keepdims=True))
    return d_act, jnp.sum(d_norm_f * unit_act, axis=0, keepdims=True)


def gain_rows(small_ref):
    return jnp.concatenate([small_ref[row] for row in range(4)], axis=1).astype(F32)


def half_masks():
    lane = lax.broadcasted_iota(jnp.int32, (1, BLK), 1)
    low = jnp.where(lane < 64, 1.0, 0.0)
    return bf(low), bf(1.0 - low), lane < 64


def pick_half(low_rows, high_rows):
    lane = lax.broadcasted_iota(jnp.int32, low_rows.shape, 1)
    return jnp.where(lane < 64, low_rows, high_rows)


def pack_slots():
    for row in range(4):
        for half in range(2):
            for mat in range(4):
                first = mat * INNER + half * 192
                yield 4 * half + row, slice(mat * 192, (mat + 1) * 192), slice(first, first + 192), slice(row * BLK, (row + 1) * BLK)


def unpack(pack_ref, full_ref):
    for dev, rows, feats, cols in pack_slots():
        full_ref[feats, cols] = pack_ref[dev, rows, :]


def repack(full_ref, pack_ref):
    for dev, rows, feats, cols in pack_slots():
        pack_ref[dev, rows, :] = full_ref[feats, cols]


def bucket_block(diag):
    row = lax.broadcasted_iota(jnp.int32, (BLK, BLK), 0)
    col = lax.broadcasted_iota(jnp.int32, (BLK, BLK), 1)
    rel = row - col + diag * BLK
    bucket = jnp.clip(rel, 0, 16)
    for edge in BUCKET_EDGES:
        bucket = bucket + jnp.where(rel >= edge, 1, 0)
    return rel, bucket


def build_bias(small_ref, bias_ref):
    tables = [small_ref[0].astype(F32), small_ref[4].astype(F32)]
    for diag in range(3):
        rel, bucket = bucket_block(diag)
        for head in range(6):
            pos = 3 + head % 3
            row = jnp.broadcast_to(tables[head // 3][pos:pos + 1, :], (BLK, BLK))
            vals = jnp.take_along_axis(row, bucket, axis=1, mode="promise_in_bounds")
            bias_ref[head, diag] = jnp.where(rel >= 0, vals, -jnp.inf)


def self_fwd(part_ref, pack_ref, small_ref, x_ref, x1_ref, qkv_ref, p_ref, ctx_ref, w_ref, bias_ref):
    @pl.when(pl.program_id(0) == 0)
    def _():
        unpack(pack_ref, w_ref)
        build_bias(small_ref, bias_ref)

    low, high, _ = half_masks()
    x_in = x_ref[0]
    unit_act, _ = unit_norm(x_in)
    normed = bf(unit_act * gain_rows(small_ref)[0:1])
    qkv_ref[0] = bf(nt(normed, w_ref[:3 * INNER]))
    for pair in range(PAIRS):
        lanes = pl.ds(pair * BLK, BLK)
        q_pair = qkv_ref[0, :, pl.ds(pair * BLK, BLK)]
        k_pair = qkv_ref[0, :, pl.ds(INNER + pair * BLK, BLK)]
        v_pair = qkv_ref[0, :, pl.ds(2 * INNER + pair * BLK, BLK)]
        k_heads = (k_pair * low, k_pair * high)
        v_heads = (v_pair * low, v_pair * high)
        for blk in range(3):
            keys = (blk + 1) * BLK
            q_rows = q_pair[blk * BLK:(blk + 1) * BLK]
            probs = []
            for sub in range(2):
                head = 2 * pair + sub
                bias = jnp.concatenate([bias_ref[head, blk - key_blk] for key_blk in range(blk + 1)], axis=1)
                logits = rounded(nt(q_rows, k_heads[sub][:keys])) + bias
                expd = jnp.exp(logits - jnp.max(logits, axis=1, keepdims=True))
                prob = expd * (1.0 / jnp.sum(expd, axis=1, keepdims=True))
                p_ref[0, head, :, ROW_OFF[blk]:ROW_OFF[blk] + keys] = prob
                probs.append(bf(prob))
            context = nn(jnp.concatenate(probs, axis=1), jnp.concatenate([v_heads[0][:keys], v_heads[1][:keys]], axis=0))
            ctx_ref[0, blk * BLK:(blk + 1) * BLK, lanes] = bf(context)
    x1_ref[0] = bf(x_in.astype(F32) + nn(ctx_ref[0], w_ref[3 * INNER:]))


def cross_mlp(begin, forward, part_ref, pack_ref, small_ref, x1_ref, enc_ref, *refs):
    if forward:
        _, yfull_ref, w_ref, mlp_ref, hid_ref, q_ref, kv_ref, p_ref, ctx_ref = refs
    else:
        dy_ref, *refs = refs
        if not begin:
            mlp_in_ref, gain_in_ref, _, *refs = refs
        y_ref, yfull_ref, dmid_ref, q_ref, kv_ref, p_ref, ctx_ref, dmlp_ref, dgain_ref, w_ref, mlp_ref, hid_ref, dpre_ref = refs

    @pl.when(pl.program_id(0) == 0)
    def _():
        unpack(pack_ref, w_ref)
        for half, mat, row, blk in np.ndindex(2, 2, 4, 4):
            first = 768 + 512 * mat + BLK * blk
            mlp_ref[half, mat, row * BLK:(row + 1) * BLK, blk * BLK:(blk + 1) * BLK] = pack_ref[4 * half + row, first:first + BLK, :]
        for half, row in np.ndindex(2, 4):
            mlp_ref[half, 2, :, row * BLK:(row + 1) * BLK] = pack_ref[4 * half + row, 1792:2304, :]
        if not forward:
            dmlp_ref[...] = jnp.zeros_like(dmlp_ref) if begin else mlp_in_ref[...]
            dgain_ref[...] = jnp.zeros_like(dgain_ref) if begin else gain_in_ref[...]

    low, high, _ = half_masks()
    unit_act, _ = unit_norm(x1_ref[0])
    gains = gain_rows(small_ref)
    normed = bf(unit_act * gains[1:2])
    q_ref[0] = bf(nt(normed, w_ref[:INNER]))
    kv_ref[0] = bf(nt(enc_ref[0], w_ref[INNER:3 * INNER]))
    for pair in range(PAIRS):
        lanes = pl.ds(pair * BLK, BLK)
        q_pair = q_ref[0, :, lanes]
        k_pair = kv_ref[0, :, lanes]
        v_pair = kv_ref[0, :, pl.ds(INNER + pair * BLK, BLK)]
        k_heads = (k_pair * low, k_pair * high)
        probs = []
        for sub in range(2):
            logits = rounded(nt(k_heads[sub], q_pair))
            expd = jnp.exp(logits - jnp.max(logits, axis=0, keepdims=True))
            prob = expd * (1.0 / jnp.sum(expd, axis=0, keepdims=True))
            p_ref[0, 2 * pair + sub] = prob
            probs.append(bf(prob))
        context = tn(jnp.concatenate(probs, axis=0), jnp.concatenate([v_pair * low, v_pair * high], axis=0))
        ctx_ref[0, :, lanes] = bf(context)
    mid_2 = rounded(x1_ref[0].astype(F32) + nn(ctx_ref[0], w_ref[3 * INNER:]))

    unit_3, inv_3 = unit_norm(mid_2)
    gain_3 = gains[2:3]
    normed_3 = bf(unit_3 * gain_3)
    dy = None if forward else dy_ref[0]
    out = mid_2
    d_norm = jnp.zeros((T, D), F32)
    for half in range(2):
        wi_0, wi_1, w_out = mlp_ref[half, 0], mlp_ref[half, 1], mlp_ref[half, 2]
        pre_0 = rounded(nn(normed_3, wi_0))
        pre_1 = rounded(nn(normed_3, wi_1))
        sq = pre_0 * pre_0
        tanh = jnp.tanh(GELU_C * (pre_0 + 0.044715 * (sq * pre_0)))
        cdf = 0.5 * (1.0 + tanh)
        gelu = pre_0 * cdf
        hid_ref[...] = bf(gelu * pre_1)
        out = out + nn(hid_ref[...], w_out)
        if forward:
            continue
        d_hid = rounded(nt(dy, w_out))
        slope = cdf + (0.5 * pre_0) * (1.0 - tanh * tanh) * (GELU_C * (1.0 + (3.0 * 0.044715) * sq))
        dpre_ref[:, 0:512] = bf((d_hid * pre_1) * slope)
        dpre_ref[:, 512:1024] = bf(d_hid * gelu)
        d_norm = d_norm + nt(dpre_ref[:, 0:512], wi_0) + nt(dpre_ref[:, 512:1024], wi_1)
        grad_in = tn(normed_3, dpre_ref[...])
        grad_out = tn(hid_ref[...], dy)
        for row in range(4):
            rows = slice(row * BLK, (row + 1) * BLK)
            for blk in range(8):
                cols = slice(blk * BLK, (blk + 1) * BLK)
                dmlp_ref[4 * half + row, cols, :] += grad_in[rows, cols]
            dmlp_ref[4 * half + row, 1024:1536, :] += grad_out[:, rows]
    if forward:
        yfull_ref[0] = bf(out)
        return
    y_ref[0] = bf(out)
    yfull_ref[0] = y_ref[0]
    d_act, d_gain = norm_back(d_norm, unit_3, inv_3, gain_3)
    dgain_ref[...] += jnp.broadcast_to(d_gain, (8, D))
    dmid_ref[0] = bf(dy.astype(F32) + d_act)


def cross_bwd(begin, part_ref, pack_ref, small_ref, x1_ref, enc_ref, dmid_ref, q_ref, kv_ref, p_ref, ctx_ref, *refs):
    if not begin:
        dw_in_ref, gain_in_ref, _, *refs = refs
    dx1_ref, denc_ref, dencfull_ref, dw_ref, dgain_ref, w_ref, acc_ref, dq_ref, dkv_ref, dctx_ref = refs
    step = pl.program_id(0)

    @pl.when(step == 0)
    def _():
        unpack(pack_ref, w_ref)
        if begin:
            acc_ref[...] = jnp.zeros_like(acc_ref)
        else:
            unpack(dw_in_ref, acc_ref)
        dgain_ref[...] = jnp.zeros_like(dgain_ref) if begin else gain_in_ref[...]

    low, high, _ = half_masks()
    d_mid = dmid_ref[0]
    dctx_ref[...] = bf(nt(d_mid, w_ref[3 * INNER:]))
    acc_ref[3 * INNER:] += tn(ctx_ref[0], d_mid)
    for pair in range(PAIRS):
        lanes = pl.ds(pair * BLK, BLK)
        q_pair = q_ref[0, :, lanes]
        k_pair = kv_ref[0, :, lanes]
        v_pair = kv_ref[0, :, pl.ds(INNER + pair * BLK, BLK)]
        dctx_pair = dctx_ref[:, lanes]
        v_heads = (v_pair * low, v_pair * high)
        probs, d_logits = [], []
        for sub in range(2):
            prob = p_ref[0, 2 * pair + sub]
            d_prob = rounded(nt(v_heads[sub], dctx_pair))
            delta = jnp.sum(prob * d_prob, axis=0, keepdims=True)
            d_logits.append(bf(prob * (d_prob - delta)))
            probs.append(bf(prob))
        d_logit = jnp.concatenate(d_logits, axis=0)
        dq_ref[:, lanes] = bf(tn(d_logit, jnp.concatenate([k_pair * low, k_pair * high], axis=0)))
        dk_both = nn(d_logit, q_pair)
        dkv_ref[:, lanes] = bf(pick_half(dk_both[:E], dk_both[E:]))
        dv_both = nn(jnp.concatenate(probs, axis=0), dctx_pair)
        dkv_ref[:, pl.ds(INNER + pair * BLK, BLK)] = bf(pick_half(dv_both[:E], dv_both[E:]))
    denc_ref[0] = bf(nn(dkv_ref[...], w_ref[INNER:3 * INNER]))
    dencfull_ref[0] = denc_ref[0]
    acc_ref[INNER:3 * INNER] += tn(dkv_ref[...], enc_ref[0])
    unit_act, inv_rms = unit_norm(x1_ref[0])
    gain = gain_rows(small_ref)[1:2]
    acc_ref[:INNER] += tn(dq_ref[...], bf(unit_act * gain))
    d_act, d_gain = norm_back(nn(dq_ref[...], w_ref[:INNER]), unit_act, inv_rms, gain)
    dgain_ref[...] += jnp.broadcast_to(d_gain, (8, D))
    dx1_ref[0] = bf(d_mid.astype(F32) + d_act)

    @pl.when(step == pl.num_programs(0) - 1)
    def _():
        repack(acc_ref, dw_ref)


def add_small(dg1_ref, dg2_ref, dg3_ref, dbias_ref, dw_ref):
    blocks = [bucket_block(diag) for diag in range(3)]
    buckets = [jnp.where(rel >= 0, bucket, -1) for rel, bucket in blocks]
    lane = lax.broadcasted_iota(jnp.int32, (8, BLK), 1)

    def one_bucket(bucket_no, sums):
        rows = []
        for head in range(6):
            total = jnp.zeros((BLK, BLK), F32)
            for diag in range(3):
                total = total + jnp.where(buckets[diag] == bucket_no, dbias_ref[head, diag], 0.0)
            rows.append(jnp.sum(total, axis=0, keepdims=True))
        rows += [jnp.zeros((1, BLK), F32)] * 2
        per_head = jnp.sum(jnp.concatenate(rows, axis=0), axis=1, keepdims=True)
        return jnp.where(lane == bucket_no, per_head, sums)

    sums = lax.fori_loop(0, NUM_BUCKETS, one_bucket, jnp.zeros((8, BLK), F32))
    gains = [ref[...] for ref in (dg1_ref, dg2_ref, dg3_ref)]
    for half in range(2):
        for row in range(4):
            parts = [gain[0:1, row * BLK:(row + 1) * BLK] for gain in gains]
            parts += [sums[3 * half:3 * half + 3], jnp.zeros((2, BLK), F32)]
            dw_ref[4 * half + row, 1536:1544, :] = jnp.concatenate(parts, axis=0)


def self_bwd(begin, part_ref, pack_ref, small_ref, x_ref, dmid_ref, qkv_ref, p_ref, ctx_ref, *refs):
    if not begin:
        dw_in_ref, gain_in_ref, bias_in_ref, dcross_ref, dg2_ref, dg3_ref, _, *refs = refs
    dx_ref, dxfull_ref, dw_ref, dgain_ref, dbias_ref, w_ref, acc_ref, dqkv_ref, dctx_ref = refs
    step = pl.program_id(0)

    @pl.when(step == 0)
    def _():
        unpack(pack_ref, w_ref)
        if begin:
            acc_ref[...] = jnp.zeros_like(acc_ref)
        else:
            unpack(dw_in_ref, acc_ref)
        dgain_ref[...] = jnp.zeros_like(dgain_ref) if begin else gain_in_ref[...]
        dbias_ref[...] = jnp.zeros_like(dbias_ref) if begin else bias_in_ref[...]

    low, high, _ = half_masks()
    d_mid = dmid_ref[0]
    dctx_ref[...] = bf(nt(d_mid, w_ref[3 * INNER:]))
    acc_ref[3 * INNER:] += tn(ctx_ref[0], d_mid)
    for pair in range(PAIRS):
        q_pair = qkv_ref[0, :, pl.ds(pair * BLK, BLK)]
        k_pair = qkv_ref[0, :, pl.ds(INNER + pair * BLK, BLK)]
        v_pair = qkv_ref[0, :, pl.ds(2 * INNER + pair * BLK, BLK)]
        dctx_pair = dctx_ref[:, pl.ds(pair * BLK, BLK)]
        k_heads = (k_pair * low, k_pair * high)
        v_heads = (v_pair * low, v_pair * high)
        probs, d_logits = [[], []], [[], []]
        for blk in range(3):
            keys = (blk + 1) * BLK
            for sub in range(2):
                head = 2 * pair + sub
                prob = p_ref[0, head, :, ROW_OFF[blk]:ROW_OFF[blk] + keys]
                d_prob = rounded(nt(dctx_pair[blk * BLK:(blk + 1) * BLK], v_heads[sub][:keys]))
                delta = jnp.sum(prob * d_prob, axis=1, keepdims=True)
                d_logit = prob * (d_prob - delta)
                for key_blk in range(blk + 1):
                    dbias_ref[head, blk - key_blk] += d_logit[:, key_blk * BLK:(key_blk + 1) * BLK]
                d_logits[sub].append(bf(d_logit))
                probs[sub].append(bf(prob))
            d_query = nn(jnp.concatenate([d_logits[0][blk], d_logits[1][blk]], axis=1),
                         jnp.concatenate([k_heads[0][:keys], k_heads[1][:keys]], axis=0))
            dqkv_ref[blk * BLK:(blk + 1) * BLK, pl.ds(pair * BLK, BLK)] = bf(d_query)
        for vals, rhs, base in ((d_logits, q_pair, INNER), (probs, dctx_pair, 2 * INNER)):
            for key_blk in range(3):
                cols = slice(key_blk * BLK, (key_blk + 1) * BLK)
                left = jnp.concatenate([jnp.concatenate([vals[sub][blk][:, cols] for blk in range(key_blk, 3)], axis=0) for sub in range(2)], axis=1)
                both = tn(left, rhs[key_blk * BLK:])
                dqkv_ref[cols, pl.ds(base + pair * BLK, BLK)] = bf(pick_half(both[:BLK], both[BLK:]))
    unit_act, inv_rms = unit_norm(x_ref[0])
    gain = gain_rows(small_ref)[0:1]
    acc_ref[:3 * INNER] += tn(dqkv_ref[...], bf(unit_act * gain))
    d_act, d_gain = norm_back(nn(dqkv_ref[...], w_ref[:3 * INNER]), unit_act, inv_rms, gain)
    dgain_ref[...] += jnp.broadcast_to(d_gain, (8, D))
    dx_ref[0] = bf(d_mid.astype(F32) + d_act)
    dxfull_ref[0] = dx_ref[0]

    @pl.when(step == pl.num_programs(0) - 1)
    def _():
        repack(acc_ref, dw_ref)
        if not begin:
            dw_ref[:, 768:1536, :] = dcross_ref[...]
            dw_ref[:, 1544:ROWS, :] = jnp.zeros((8, ROWS - 1544, BLK), F32)
            add_small(dgain_ref, dg2_ref, dg3_ref, dbias_ref, dw_ref)


def seq_block(first, *dims):
    zeros = (0,) * len(dims)
    return pl.BlockSpec((1,) + dims, lambda i, part: (first + i,) + zeros)


def arg_block(first, *dims):
    zeros = (0,) * len(dims)
    return pl.BlockSpec((1,) + dims, lambda i, part: (part[0] * 8 + first + i,) + zeros)


def other_block(first, *dims):
    zeros = (0,) * len(dims)
    return pl.BlockSpec((1,) + dims, lambda i, part: ((1 - part[0]) * 8 + first + i,) + zeros)


def whole(*dims):
    zeros = (0,) * len(dims)
    return pl.BlockSpec(dims, lambda i, part: zeros)


def shape(dims, dtype):
    return jax.ShapeDtypeStruct(dims, dtype)


def whole_out(dims, dtype):
    return whole(*dims), shape(dims, dtype)


def call(body, seqs, flops, in_specs, outs, scratch, args, aliases=None):
    out_specs, out_shape = zip(*outs)
    return pl.pallas_call(
        body,
        out_shape=out_shape,
        grid_spec=pltpu.PrefetchScalarGridSpec(num_scalar_prefetch=1, grid=(seqs,), in_specs=in_specs, out_specs=out_specs, scratch_shapes=scratch),
        input_output_aliases=aliases or {},
        compiler_params=pltpu.CompilerParams(dimension_semantics=("arbitrary",), vmem_limit_bytes=VMEM_LIMIT),
        cost_estimate=pl.CostEstimate(flops=flops * seqs, bytes_accessed=5_000_000 * seqs, transcendentals=0),
    )(*args)


def stack_cols(weight):
    return [weight.reshape(BLK, 4, BLK).transpose(1, 0, 2).reshape(512, BLK)]


def layer_shard(dec_in, enc_out, grad_out, rel_bias, self_q, self_k, self_v, self_o, cross_q, cross_k, cross_v, cross_o, mlp_wi_0, mlp_wi_1, mlp_wo, norm_self, norm_cross, norm_mlp):
    axes = ("model", "data")
    batch = dec_in.shape[0]
    seqs = batch // 2
    chunk = seqs // 2
    part = lax.axis_index("model").astype(jnp.int32).reshape(1)
    rows = (norm_self[None], norm_cross[None], norm_mlp[None], jnp.pad(rel_bias.T, ((0, 0), (0, BLK - NUM_BUCKETS))))
    small = sum(jnp.pad(val, ((pos, 16 - pos - val.shape[0]), (0, 0))) for pos, val in enumerate(rows))
    w_self = lax.all_gather(jnp.concatenate([self_q.T, self_k.T, self_v.T, self_o, small], axis=0), axes)
    w_rest = lax.all_gather(jnp.concatenate([cross_q.T, cross_k.T, cross_v.T, cross_o] + stack_cols(mlp_wi_0) + stack_cols(mlp_wi_1) + [mlp_wo], axis=0), axes)

    vmem = pltpu.VMEM
    pack_spec = whole(8, 768, BLK)
    small_spec = pl.BlockSpec((8, 16, BLK), lambda i, part: (0, 48, 0))
    any_spec = pl.BlockSpec(memory_space=pl.ANY)
    w_scr = vmem((1536, D), BF)
    acc_scr = vmem((1536, D), F32)
    full_out = {rows: shape((batch, rows, D), BF) for rows in (T, E)}
    model_no = lax.axis_index("model")

    def seq_out(count, dims, dtype):
        return seq_block(0, *dims), shape((count,) + dims, dtype)

    def send(val):
        return lax.ppermute(val, "model", [(0, 1), (1, 0)])

    def scatter(val):
        return lax.psum_scatter(val, axes, scatter_dimension=0)

    def place(full, received):
        for pos, val in enumerate(received):
            full = lax.dynamic_update_slice(full, val, ((1 - model_no) * seqs + pos * chunk, 0, 0))
        return full

    mid_1, qkv, probs, ctx = call(
        self_fwd, seqs, 7_000_000_000,
        [pack_spec, small_spec, arg_block(0, T, D)],
        [seq_out(seqs, (T, D), BF), seq_out(seqs, (T, 3 * INNER), BF), seq_out(seqs, (6, BLK, 768), F32), seq_out(seqs, (T, INNER), BF)],
        [w_scr, vmem((6, 3, BLK, BLK), F32)],
        (part, w_self, w_self, dec_in))

    saved, got_y, chain = [], [], ()
    for pos in range(2):
        first = pos * chunk
        extra = [whole(8, 1536, BLK), whole(8, D), any_spec] if pos else []
        y_part, y_full, d_mid, q_x, kv_x, probs_x, ctx_x, d_mlp, d_gain_3 = call(
            functools.partial(cross_mlp, pos == 0, False), chunk, 14_000_000_000,
            [whole(8, 2304, BLK), small_spec, seq_block(first, T, D), arg_block(first, E, D), arg_block(first, T, D)] + extra,
            [seq_out(chunk, (T, D), BF), (arg_block(first, T, D), full_out[T]), seq_out(chunk, (T, D), BF), seq_out(chunk, (T, INNER), BF), seq_out(chunk, (E, 2 * INNER), BF),
             seq_out(chunk, (6, E, T), F32), seq_out(chunk, (T, INNER), BF), whole_out((8, 1536, BLK), F32), whole_out((8, D), F32)],
            [w_scr, vmem((2, 3, 512, 512), BF), vmem((T, 512), BF), vmem((T, 1024), BF)],
            (part, w_rest, w_self, mid_1, enc_out, grad_out) + chain, {8: 1} if pos else None)
        chain = (d_mlp, d_gain_3, y_full)
        if pos == 0:
            got_y.append(send(y_part))
        saved.append((d_mid, q_x, kv_x, probs_x, ctx_x))
    d_mlp = scatter(d_mlp)

    d_mids, got_e, chain = [], [], ()
    for pos in range(2):
        first = pos * chunk
        extra = [pack_spec, whole(8, D), any_spec] if pos else []
        d_mid_1, e_part, e_full, d_cross, d_gain_2 = call(
            functools.partial(cross_bwd, pos == 0), chunk, 7_000_000_000,
            [pack_spec, small_spec, seq_block(first, T, D), arg_block(first, E, D), seq_block(0, T, D), seq_block(0, T, INNER), seq_block(0, E, 2 * INNER), seq_block(0, 6, E, T), seq_block(0, T, INNER)] + extra,
            [seq_out(chunk, (T, D), BF), seq_out(chunk, (E, D), BF), (arg_block(first, E, D), full_out[E]), whole_out((8, 768, BLK), F32), whole_out((8, D), F32)],
            [w_scr, acc_scr, vmem((T, INNER), BF), vmem((E, 2 * INNER), BF), vmem((T, INNER), BF)],
            (part, w_rest, w_self, mid_1, enc_out) + saved[pos] + chain, {12: 2} if pos else None)
        chain = (d_cross, d_gain_2, e_full)
        got_e.append(send(e_part))
        d_mids.append(d_mid_1)

    got_x, chain = [], ()
    for pos in range(2):
        first = pos * chunk
        extra = [pack_spec, whole(8, D), whole(6, 3, BLK, BLK), pack_spec, whole(8, D), whole(8, D), any_spec] if pos else []
        x_part, x_full, d_self, d_gain_1, d_bias = call(
            functools.partial(self_bwd, pos == 0), chunk, 11_000_000_000,
            [pack_spec, small_spec, arg_block(first, T, D), seq_block(0, T, D), seq_block(first, T, 3 * INNER), seq_block(first, 6, BLK, 768), seq_block(first, T, INNER)] + extra,
            [seq_out(chunk, (T, D), BF), (arg_block(first, T, D), full_out[T]), whole_out((8, ROWS if pos else 768, BLK), F32), whole_out((8, D), F32), whole_out((6, 3, BLK, BLK), F32)],
            [w_scr, acc_scr, vmem((T, 3 * INNER), BF), vmem((T, INNER), BF)],
            (part, w_self, w_self, dec_in, d_mids[pos], qkv, probs, ctx) + chain, {14: 1} if pos else None)
        chain = (d_self, d_gain_1, d_bias, d_cross, d_gain_2, d_gain_3, x_full)
        got_x.append(send(x_part))
    d_self = scatter(d_self)

    mid_other, _, _, _ = call(
        self_fwd, chunk, 7_000_000_000,
        [pack_spec, small_spec, other_block(chunk, T, D)],
        [seq_out(chunk, (T, D), BF), seq_out(chunk, (T, 3 * INNER), BF), seq_out(chunk, (6, BLK, 768), F32), seq_out(chunk, (T, INNER), BF)],
        [w_scr, vmem((6, 3, BLK, BLK), F32)],
        (part, w_self, w_self, dec_in))
    y_full, = call(
        functools.partial(cross_mlp, False, True), chunk, 7_000_000_000,
        [whole(8, 2304, BLK), small_spec, seq_block(0, T, D), other_block(chunk, E, D), any_spec],
        [(other_block(chunk, T, D), full_out[T])],
        [w_scr, vmem((2, 3, 512, 512), BF), vmem((T, 512), BF), vmem((1, T, INNER), BF), vmem((1, E, 2 * INNER), BF), vmem((1, 6, E, T), F32), vmem((1, T, INNER), BF)],
        (part, w_rest, w_self, mid_other, enc_out, y_full), {5: 0})

    gain_grads = (d_self[1536], d_self[1537], d_self[1538])
    grad_bias = d_self[1539:1542, :NUM_BUCKETS].T
    dec_out, grad_enc, grad_dec = place(y_full, got_y), place(e_full, got_e), place(x_full, got_x)

    def split_attn(grad_pack):
        mats = [grad_pack[192 * pos:192 * (pos + 1)] for pos in range(4)]
        return mats[0].T, mats[1].T, mats[2].T, mats[3]

    def join_cols(rows):
        return jnp.concatenate([rows[blk * BLK:(blk + 1) * BLK] for blk in range(4)], axis=1)

    return (dec_out, grad_dec, grad_enc, grad_bias) + split_attn(d_self) + split_attn(d_self[768:]) + (
        join_cols(d_mlp[:512]), join_cols(d_mlp[512:1024]), d_mlp[1024:]) + gain_grads


def solution(mesh):
    row_spec = P("data", None, None)
    col_in = P("data", "model")
    col_out = P("model", "data")
    gain_spec = P("data")
    bias_spec = P(None, "model")
    arg_specs = (row_spec, row_spec, row_spec, bias_spec, col_in, col_in, col_in, col_out, col_in, col_in, col_in, col_out, col_in, col_in, col_out, gain_spec, gain_spec, gain_spec)
    out_specs = (row_spec, row_spec, row_spec) + arg_specs[3:]

    return jax.shard_map(layer_shard, mesh=mesh, in_specs=arg_specs, out_specs=out_specs, check_vma=False)
```
